256 devices in a mesh: walk: 32 (over z, x), chol: 8 (over y, core).
Axes of the slice: x: 4, y: 4, z: 8, core: 2. Of those that a mesh axis runs over, the one named last changes fastest.
Arguments:
- orbitals: bfloat16 [32, 400, 2048], P('walk', None, 'chol'), may hold values from -4 to 4
- intersection_inv: bfloat16 [32, 400, 400], P('walk'), may hold values from -0.18 to 0.18
- interp: bfloat16 [2048, 4096], P(None, 'chol'), may hold values from -0.079549513 to 0.079549513
- occ_interp: bfloat16 [400, 4096], P(None, 'chol'), may hold values from -0.18 to 0.18
- chol_factors: bfloat16 [4096, 8192], P('chol', 'walk'), may hold values from -2 to 2
- fields: float32 [32, 8192], P(None, 'walk'), may hold values from -4 to 4
Outputs:
- new_orbitals: bfloat16 [32, 400, 2048], P('walk', None, 'chol')
- force_bias: float32 [32, 8192], P(None, 'walk')
The draws below stay inside these ranges and needn't reach their ends.
All inputs are finite; a program needn't handle non-finite values.
Results may differ from the reference program's by a relative error of at most 0.017.
Values may be sent and summed in bfloat16 or wider, within the bound.
A program may use at most 64 MiB of HBM per device.

```python
import jax
import jax.numpy as jnp
from jax import lax

BASIS_SIZE = 2048
ELECTRONS = 400
PTS_DEV = 512
TERMS = 4
POINTS = 4096
VECTORS = 8192
WALKERS = 32
N_CHOL = 8


def bounded_values(key, shape, deviation):
    base = jax.random.truncated_normal(key, -3.5, 3.5, shape, jnp.float32)
    return base * deviation


def draw_orbitals(key, part):
    values = bounded_values(jax.random.fold_in(key, 11), (WALKERS, ELECTRONS, BASIS_SIZE), 1.0)
    return values.astype(jnp.bfloat16)


def draw_intersection_inv(key, part):
    deviation = 1.0 / jnp.sqrt(jnp.float32(ELECTRONS))
    values = bounded_values(jax.random.fold_in(key, 13), (WALKERS, ELECTRONS, ELECTRONS), deviation)
    return values.astype(jnp.bfloat16)


def draw_interp(key, part):
    deviation = 1.0 / jnp.sqrt(jnp.float32(BASIS_SIZE))
    values = bounded_values(jax.random.fold_in(key, 17), (BASIS_SIZE, POINTS), deviation)
    return values.astype(jnp.bfloat16)


def draw_occ_interp(key, part):
    deviation = 1.0 / jnp.sqrt(jnp.float32(ELECTRONS))
    values = bounded_values(jax.random.fold_in(key, 19), (ELECTRONS, POINTS), deviation)
    return values.astype(jnp.bfloat16)


def draw_fields(key, part):
    return bounded_values(jax.random.fold_in(key, 23), (WALKERS, VECTORS), 1.0)


def draw_chol_factors(key, part):
    first_key, second_key = jax.random.split(jax.random.fold_in(key, 7))
    column = jnp.arange(VECTORS).astype(jnp.float32) / VECTORS
    spread = jax.random.uniform(second_key, (VECTORS,), jnp.float32)
    column_scale = 0.2 * 10.0 ** (0.5 * column + 0.5 * spread)
    base = jax.random.truncated_normal(first_key, -4.0, 4.0, (POINTS, VECTORS), jnp.float32)
    normalizer = 0.75 * jnp.sqrt(jnp.float32(BASIS_SIZE) / (jnp.float32(POINTS) * jnp.float32(VECTORS)))
    values = base * column_scale[None, :] * normalizer
    return values.astype(jnp.bfloat16)


def setup_inputs(seed: int = 0) -> dict:
    key_of = jax.random.split(jax.random.key(seed), 7)
    return {
        "orbitals": draw_orbitals(jax.random.fold_in(key_of[6], 71), 0),
        "intersection_inv": draw_intersection_inv(jax.random.fold_in(key_of[6], 71), 0),
        "interp": draw_interp(jax.random.fold_in(key_of[6], 71), 0),
        "occ_interp": draw_occ_interp(jax.random.fold_in(key_of[6], 71), 0),
        "chol_factors": draw_chol_factors(jax.random.fold_in(key_of[6], 71), 0),
        "fields": draw_fields(jax.random.fold_in(key_of[6], 71), 0),
    }


time_root = 2.2


def propagate(orbit, inverse, field_row, interp, occ_interp, chol_factors):
    green = jnp.dot(inverse, orbit, preferred_element_type=jnp.float32).astype(jnp.bfloat16)
    projected = jnp.dot(green, interp, preferred_element_type=jnp.float32)
    weights = jnp.sum(occ_interp.astype(jnp.float32) * projected, axis=0)
    factors = chol_factors.astype(jnp.float32)
    bias = jnp.dot(weights, factors, precision=lax.Precision.HIGHEST)
    coeff = time_root * (field_row - bias)
    scales = jnp.dot(factors, coeff, precision=lax.Precision.HIGHEST)
    total = orbit.astype(jnp.float32)
    term = orbit
    for order in range(1, TERMS + 1):
        product = jnp.dot(term, interp, preferred_element_type=jnp.float32)
        mixed = (product * scales[None, :] / order).astype(jnp.bfloat16)
        summed = jnp.zeros(orbit.shape, jnp.float32)
        for block in range(N_CHOL):
            lower = block * PTS_DEV
            piece = jnp.dot(mixed[:, lower:lower + PTS_DEV], interp[:, lower:lower + PTS_DEV].T, preferred_element_type=jnp.float32)
            rounded = lax.optimization_barrier(piece.astype(jnp.bfloat16))
            summed = summed + rounded.astype(jnp.float32)
        term = summed.astype(jnp.bfloat16)
        total = total + term.astype(jnp.float32)
    return total.astype(jnp.bfloat16), bias


def reference(orbitals, intersection_inv, interp, occ_interp, chol_factors, fields):
    def single(items):
        return propagate(items[0], items[1], items[2], interp, occ_interp, chol_factors)

    new_orbitals, force_bias = lax.map(single, (orbitals, intersection_inv, fields))
    return (new_orbitals, force_bias)
```

```python
import jax
import jax.numpy as jnp
from jax import lax
from jax.experimental import pallas as pl
from jax.experimental.pallas import tpu as pltpu
from jax.sharding import PartitionSpec as P

TERMS = 4
TIME_ROOT = 2.2
MESH = pl.DeviceIdType.MESH
F32, BF16 = jnp.float32, jnp.bfloat16

NX, NZ, NY = 4, 8, 4
WALK, CHOL = NX * NZ, NY * 2
ROWS, BASIS, PTS, VEC = 400, 2048, 512, 256
COLS = BASIS // CHOL
WIN, STEP = 112, 96
XROWS, ZROWS = 256, 128
ZBASE = NX * XROWS
TILE = 512
TILES = BASIS // TILE


def three_parts(value):
    high = value.astype(BF16)
    rest = value - high.astype(F32)
    middle = rest.astype(BF16)
    low = (rest - middle.astype(F32)).astype(BF16)
    return jnp.concatenate([high, middle, low], axis=0)


def sum_of_parts(value, rows):
    return value[:rows] + value[rows : 2 * rows] + value[2 * rows :]


def dot(left, right):
    return jnp.dot(left, right, preferred_element_type=F32)


def dot_last(left, right):
    return lax.dot_general(left, right, (((1,), (1,)), ((), ())), preferred_element_type=F32)


def kernel(
    orb_in, inv_in, interp_in, occ_in, chol_in, fields_in,
    out, bias_out,
    ip, orb, inv, occ, chol, fields,
    gathered, product, weights, bias_parts, bias, field_part, scale_in, scales,
    current, mixed, own_part, other_part, term, total, send_out, recv_out,
    load_sem, gather_send, gather_recv, orb_send, orb_recv,
    small_send, small_recv, part_send, part_recv, out_send, out_recv, store_sem,
):
    walk, place = lax.axis_index("walk"), lax.axis_index("chol")
    x, z = lax.rem(walk, NX), lax.div(walk, NX)
    core, y = lax.rem(place, 2), lax.div(place, 2)

    def at_y(step):
        return lax.rem(y + step + NY, NY)

    def chol_of(step):
        return at_y(step) * 2 + core

    def on_x(step):
        return {"walk": z * NX + lax.rem(x + step + NX, NX), "chol": place}

    def on_z(step):
        return {"walk": lax.rem(z + step + NZ, NZ) * NX + x, "chol": place}

    def on_y(step):
        return {"walk": walk, "chol": chol_of(step)}

    partner = {"walk": walk, "chol": y * 2 + (1 - core)}

    barrier = pltpu.get_barrier_semaphore()

    def greet_walk(step, carry):
        pl.semaphore_signal(
            barrier, inc=1,
            device_id={"walk": lax.rem(walk + step, WALK), "chol": place}, device_id_type=MESH,
        )
        return carry

    def greet_chol(step, carry):
        pl.semaphore_signal(
            barrier, inc=1,
            device_id={"walk": walk, "chol": lax.rem(place + step, CHOL)}, device_id_type=MESH,
        )
        return carry

    lax.fori_loop(1, WALK, greet_walk, 0)
    lax.fori_loop(1, CHOL, greet_chol, 0)
    loads = [
        pltpu.make_async_copy(orb_in.at[0], orb.at[place], load_sem.at[0]),
        pltpu.make_async_copy(interp_in, ip.at[y], load_sem.at[1]),
        pltpu.make_async_copy(inv_in.at[0], inv, load_sem.at[2]),
        pltpu.make_async_copy(occ_in, occ, load_sem.at[3]),
        pltpu.make_async_copy(chol_in, chol, load_sem.at[4]),
        pltpu.make_async_copy(fields_in, fields, load_sem.at[5]),
    ]
    for load in loads:
        load.start()
    loads[2].wait()
    loads[3].wait()
    gathered[...] = lax.dot_general(
        inv[...], occ[...], (((0,), (0,)), ((), ())), preferred_element_type=F32
    )
    loads[0].wait()
    loads[1].wait()
    loads[4].wait()
    loads[5].wait()
    pl.semaphore_wait(barrier, WALK - 1 + CHOL - 1)

    def moved(index, block, start, count, device):
        place_of = ip.at[block, pl.ds(pl.multiple_of(start, 16), count)]
        return pltpu.make_async_remote_copy(
            src_ref=place_of, dst_ref=place_of,
            send_sem=gather_send.at[index], recv_sem=gather_recv.at[index],
            device_id=device, device_id_type=MESH,
        )

    transfers = {}

    def start_gather(name, *what):
        copy = moved(len(transfers), *what)
        transfers[name] = copy
        copy.start()

    def landed(*names):
        for name in names:
            transfers[name].wait_recv()

    x_start = x * XROWS
    z_start = ZBASE + z * ZROWS

    def x_piece(step):
        return lax.rem(x + step + NX, NX) * XROWS

    def z_piece(step):
        return ZBASE + lax.rem(z + step + NZ, NZ) * ZROWS

    def y0(kind):
        start, count = (x_start, XROWS) if kind == "x" else (z_start, ZROWS)
        for way in (1, -1):
            start_gather(("y0", kind, way), y, start, count, on_y(way))

    def y1(kind):
        start, count = (x_start, XROWS) if kind == "x" else (z_start, ZROWS)
        half = count // 2
        start_gather(("y1", kind, 1), at_y(-1), start, half, on_y(1))
        start_gather(("y1", kind, -1), at_y(1), start + half, half, on_y(-1))

    def x0(block):
        for way in (1, -1):
            start_gather(("x0", block, way), at_y(block), x_start, XROWS, on_x(way))

    def x1(block):
        half = XROWS // 2
        start_gather(("x1", block, 1), at_y(block), x_piece(-1), half, on_x(1))
        start_gather(("x1", block, -1), at_y(block), x_piece(1) + half, half, on_x(-1))

    def zs(step, block):
        for way in (1, -1):
            start_gather(
                (f"z{step}", block, way), at_y(block), z_piece(-way * step), ZROWS, on_z(way)
            )

    def z3(block):
        half = ZROWS // 2
        start_gather(("z3", block, 1), at_y(block), z_piece(-3), half, on_z(1))
        start_gather(("z3", block, -1), at_y(block), z_piece(3) + half, half, on_z(-1))

    def both(stage, block):
        landed((stage, block, 1), (stage, block, -1))

    def orb_copy(index, block, rows, device):
        place_of = orb.at[block, rows]
        return pltpu.make_async_remote_copy(
            src_ref=place_of, dst_ref=place_of,
            send_sem=orb_send.at[index], recv_sem=orb_recv.at[index],
            device_id=device, device_id_type=MESH,
        )

    everything, lower, upper = pl.ds(0, ROWS), pl.ds(0, 208), pl.ds(208, 192)
    o_up = orb_copy(0, place, everything, on_y(1))
    o_down = orb_copy(1, place, everything, on_y(-1))
    o_across = orb_copy(2, place, everything, partner)
    o_up.start()
    o_down.start()
    o_across.start()
    y0("z")

    def other(block):
        return lax.div(block, 2) * 2 + (1 - lax.rem(block, 2))

    def add_product(block, first=False):
        part = dot(orb[block], ip[y, pl.ds(pl.multiple_of(block * COLS, COLS), COLS), :])
        product[...] = part if first else product[...] + part

    below, above, far = chol_of(-1), chol_of(1), chol_of(2)
    add_product(place, True)
    o_up.wait_recv()
    o_up2 = orb_copy(3, below, lower, on_y(1))
    o_up2.start()
    o_across_below = orb_copy(4, below, everything, partner)
    o_across_below.start()
    o_down.wait_recv()
    o_down2 = orb_copy(5, above, upper, on_y(-1))
    o_down2.start()
    o_across_above = orb_copy(6, above, everything, partner)
    o_across_above.start()
    y0("x")
    o_across.wait_recv()
    add_product(other(place))
    add_product(below)
    add_product(above)
    landed(("y0", "z", 1), ("y0", "z", -1))
    zs(0, -1)
    zs(0, 1)
    y1("z")
    o_across_below.wait_recv()
    add_product(other(below))
    o_across_above.wait_recv()
    add_product(other(above))
    o_up2.wait_recv()
    o_down2.wait_recv()
    o_across_far = orb_copy(7, far, everything, partner)
    o_across_far.start()
    add_product(far)
    o_across_far.wait_recv()
    add_product(other(far))

    weights[walk] = jnp.sum(gathered[...] * product[...], axis=0, keepdims=True)

    def send_weights(step, carry):
        pltpu.make_async_remote_copy(
            src_ref=weights.at[walk], dst_ref=weights.at[walk],
            send_sem=small_send.at[0], recv_sem=small_recv.at[0],
            device_id={"walk": lax.rem(walk + step, WALK), "chol": place}, device_id_type=MESH,
        ).start()
        return carry

    lax.fori_loop(1, WALK, send_weights, 0)
    landed(("y0", "x", 1), ("y0", "x", -1))
    x0(-1)
    x0(1)
    y1("x")
    both("z0", -1)
    zs(1, -1)
    both("z0", 1)
    zs(1, 1)
    landed(("y1", "z", 1), ("y1", "z", -1))
    zs(0, 2)
    some = weights.at[pl.ds(0, WALK - 1)]
    pltpu.make_async_copy(some, some, small_recv.at[0]).wait()

    all_weights = weights[...].reshape(WALK, PTS)
    partial = sum_of_parts(dot(three_parts(all_weights), chol[...]), WALK)
    bias_parts[place] = partial

    def send_bias(step, carry):
        pltpu.make_async_remote_copy(
            src_ref=bias_parts.at[place], dst_ref=bias_parts.at[place],
            send_sem=small_send.at[1], recv_sem=small_recv.at[1],
            device_id={"walk": walk, "chol": lax.rem(place + step, CHOL)}, device_id_type=MESH,
        ).start()
        return carry

    lax.fori_loop(1, CHOL, send_bias, 0)
    both("z1", -1)
    zs(2, -1)
    both("z1", 1)
    zs(2, 1)
    both("x0", -1)
    x1(-1)
    landed(("y1", "x", 1), ("y1", "x", -1))
    x0(2)
    both("x0", 1)
    x1(1)
    some_bias = bias_parts.at[pl.ds(0, CHOL - 1)]
    pltpu.make_async_copy(some_bias, some_bias, small_recv.at[1]).wait()
    bias[...] = jnp.sum(bias_parts[...], axis=0)
    store_bias = pltpu.make_async_copy(bias, bias_out, store_sem.at[0])
    store_bias.start()

    coeff = TIME_ROOT * (fields[...] - bias[...])
    part = sum_of_parts(dot_last(three_parts(coeff), chol[...]), WALK)
    field_part[...] = part.reshape(WALK, 1, PTS)

    def send_scales(step, carry):
        to = lax.rem(walk + step, WALK)
        pltpu.make_async_remote_copy(
            src_ref=field_part.at[to], dst_ref=scale_in.at[walk],
            send_sem=small_send.at[2], recv_sem=small_recv.at[2],
            device_id={"walk": to, "chol": place}, device_id_type=MESH,
        ).start()
        return carry

    lax.fori_loop(1, WALK, send_scales, 0)
    scale_in[walk] = field_part[walk]
    both("z0", 2)
    zs(1, 2)
    both("z2", -1)
    z3(-1)
    both("z2", 1)
    z3(1)
    both("x0", 2)
    x1(2)
    some_scales = scale_in.at[pl.ds(0, WALK - 1)]
    pltpu.make_async_copy(some_scales, some_scales, small_recv.at[2]).wait()
    scales[y] = jnp.sum(scale_in[...], axis=0)
    to_up = [
        pltpu.make_async_remote_copy(
            src_ref=scales.at[y], dst_ref=scales.at[y],
            send_sem=small_send.at[3], recv_sem=small_recv.at[3],
            device_id=on_y(step), device_id_type=MESH,
        )
        for step in range(1, NY)
    ]
    for copy in to_up:
        copy.start()

    both("z1", 2)
    zs(2, 2)
    both("z2", 2)
    z3(2)
    both("x1", -1)
    both("x1", 1)
    both("x1", 2)
    both("z3", -1)
    both("z3", 1)
    both("z3", 2)

    window = pl.ds(pl.multiple_of(y * STEP, 16), WIN)
    for block in range(CHOL):
        rows = orb[block, window, :]
        term[:, block * COLS : (block + 1) * COLS] = rows
        total[:, block * COLS : (block + 1) * COLS] = rows.astype(F32)

    def multiply(block, carry):
        current[block] = dot(term[...], ip[block])
        return carry

    lax.fori_loop(0, NY, multiply, 0)
    some_blocks = scales.at[pl.ds(0, NY - 1)]
    pltpu.make_async_copy(some_blocks, some_blocks, small_recv.at[3]).wait()

    for order in range(1, TERMS + 1):
        if order > 1:
            lax.fori_loop(0, NY, multiply, 0)
        for block in range(NY):
            mixed[:, block * PTS : (block + 1) * PTS] = (
                current[block] * scales[block] / order
            ).astype(BF16)
        slot = order - 1

        def exchange(tile):
            return pltpu.make_async_remote_copy(
                src_ref=own_part.at[slot, tile], dst_ref=other_part.at[slot, tile],
                send_sem=part_send.at[slot, tile], recv_sem=part_recv.at[slot, tile],
                device_id=partner, device_id_type=MESH,
            )

        def back(tile, carry):
            rows = pl.ds(pl.multiple_of(tile * TILE, TILE), TILE)
            value = dot_last(mixed[:, 0:PTS], ip[0, rows, :])
            for block in range(1, NY):
                value += dot_last(mixed[:, block * PTS : (block + 1) * PTS], ip[block, rows, :])
            own_part[slot, tile] = value.astype(BF16)
            exchange(tile).start()
            return carry

        lax.fori_loop(0, TILES, back, 0)
        for tile in range(TILES):
            exchange(tile).wait_recv()
            columns = slice(tile * TILE, (tile + 1) * TILE)
            value = (own_part[slot, tile].astype(F32) + other_part[slot, tile].astype(F32)).astype(BF16)
            term[:, columns] = value
            total[:, columns] = total[:, columns] + value.astype(F32)

    for step in (2, 1, 3, 0):
        to = at_y(step)
        columns = pl.ds(pl.multiple_of((to * 2 + core) * COLS, COLS), COLS)
        send_out[to] = total[:, columns].astype(BF16)
        if step:
            pltpu.make_async_remote_copy(
                src_ref=send_out.at[to], dst_ref=recv_out.at[y],
                send_sem=out_send, recv_sem=out_recv,
                device_id=on_y(step), device_id_type=MESH,
            ).start()
    recv_out[y] = send_out[y]
    some_out = recv_out.at[pl.ds(0, NY - 1)]
    pltpu.make_async_copy(some_out, some_out, out_recv).wait()
    stores = []
    for part in range(NY):
        count = WIN if part == NY - 1 else STEP
        stores.append(
            pltpu.make_async_copy(
                recv_out.at[part, pl.ds(0, count)], out.at[0, pl.ds(part * STEP, count)],
                store_sem.at[1 + part],
            )
        )
    for store in stores:
        store.start()

    for copy in transfers.values():
        copy.wait_send()
    for copy in (o_up, o_down, o_across, o_up2, o_down2, o_across_below, o_across_above, o_across_far):
        copy.wait_send()
    pltpu.make_async_copy(some, some, small_send.at[0]).wait()
    pltpu.make_async_copy(some_bias, some_bias, small_send.at[1]).wait()
    pltpu.make_async_copy(some_scales, some_scales, small_send.at[2]).wait()
    pltpu.make_async_copy(some_blocks, some_blocks, small_send.at[3]).wait()
    for slot in range(TERMS):
        for tile in range(TILES):
            pltpu.make_async_copy(
                own_part.at[slot, tile], other_part.at[slot, tile], part_send.at[slot, tile]
            ).wait()
    pltpu.make_async_copy(some_out, some_out, out_send).wait()
    store_bias.wait()
    for store in stores:
        store.wait()


N_GATHER = 8 + 12 + 24


def on_device(orbitals, intersection_inv, interp, occ_interp, chol_factors, fields):
    dma = pltpu.SemaphoreType.DMA
    hbm = pl.BlockSpec(memory_space=pl.ANY)
    return pl.pallas_call(
        kernel,
        out_shape=(
            jax.ShapeDtypeStruct((1, ROWS, COLS), BF16),
            jax.ShapeDtypeStruct((WALK, VEC), F32),
        ),
        in_specs=[hbm] * 6,
        out_specs=(hbm, hbm),
        scratch_shapes=[
            pltpu.VMEM((NY, BASIS, PTS), BF16),
            pltpu.VMEM((CHOL, ROWS, COLS), BF16),
            pltpu.VMEM((ROWS, ROWS), BF16),
            pltpu.VMEM((ROWS, PTS), BF16),
            pltpu.VMEM((PTS, VEC), BF16),
            pltpu.VMEM((WALK, VEC), F32),
            pltpu.VMEM((ROWS, PTS), F32),
            pltpu.VMEM((ROWS, PTS), F32),
            pltpu.VMEM((WALK, 1, PTS), F32),
            pltpu.VMEM((CHOL, WALK, VEC), F32),
            pltpu.VMEM((WALK, VEC), F32),
            pltpu.VMEM((WALK, 1, PTS), F32),
            pltpu.VMEM((WALK, 1, PTS), F32),
            pltpu.VMEM((NY, 1, PTS), F32),
            pltpu.VMEM((NY, WIN, PTS), F32),
            pltpu.VMEM((WIN, NY * PTS), BF16),
            pltpu.VMEM((TERMS, TILES, WIN, TILE), BF16),
            pltpu.VMEM((TERMS, TILES, WIN, TILE), BF16),
            pltpu.VMEM((WIN, BASIS), BF16),
            pltpu.VMEM((WIN, BASIS), F32),
            pltpu.VMEM((NY, WIN, COLS), BF16),
            pltpu.VMEM((NY, WIN, COLS), BF16),
            dma((6,)),
            dma((N_GATHER,)),
            dma((N_GATHER,)),
            dma((8,)),
            dma((8,)),
            dma((4,)),
            dma((4,)),
            dma((TERMS, TILES)),
            dma((TERMS, TILES)),
            dma,
            dma,
            dma((5,)),
        ],
        compiler_params=pltpu.CompilerParams(
            collective_id=0, has_side_effects=True, vmem_limit_bytes=60 * 1024 * 1024
        ),
    )(orbitals, intersection_inv, interp, occ_interp, chol_factors, fields)


def solution(mesh):
    placed = (
        P("walk", None, "chol"),
        P("walk", None, None),
        P(None, "chol"),
        P(None, "chol"),
        P("chol", "walk"),
        P(None, "walk"),
    )
    return jax.shard_map(
        on_device,
        mesh=mesh,
        in_specs=placed,
        out_specs=(P("walk", None, "chol"), P(None, "walk")),
        check_vma=False,
    )
```

```python
import jax
import jax.numpy as jnp
from jax import lax
from jax.experimental import pallas as pl
from jax.experimental.pallas import tpu as pltpu
from jax.sharding import PartitionSpec as P

TERMS = 4
TIME_ROOT = 2.2
MESH = pl.DeviceIdType.MESH
F32, BF16 = jnp.float32, jnp.bfloat16

NX, NZ, NY = 4, 8, 4
WALK, CHOL = NX * NZ, NY * 2
ROWS, BASIS, PTS, VEC = 400, 2048, 512, 256
COLS = BASIS // CHOL
WIN, STEP = 112, 96
XROWS, XHALF = 224, 112
ZROWS, ZHALF = 96, 48
ZBASE = NX * XROWS
CBASE = ZBASE + NZ * ZROWS
CROWS, CHALF = BASIS - CBASE, 192
TILE = 512
TILES = BASIS // TILE
TURN = 512


def three_parts(value):
    high = value.astype(BF16)
    rest = value - high.astype(F32)
    middle = rest.astype(BF16)
    low = (rest - middle.astype(F32)).astype(BF16)
    return jnp.concatenate([high, middle, low], axis=0)


def sum_of_parts(value, rows):
    return value[:rows] + value[rows : 2 * rows] + value[2 * rows :]


def dot(left, right):
    return jnp.dot(left, right, preferred_element_type=F32)


def dot_last(left, right):
    return lax.dot_general(left, right, (((1,), (1,)), ((), ())), preferred_element_type=F32)


def kernel(
    orb_in, inv_in, interp_in, occ_in, chol_in, fields_in,
    out, bias_out,
    ip, turned, orb, inv, occ, chol, fields,
    gathered, product, weights, pair, bias_parts, bias, field_part, scale_in, scales,
    current, mixed, own_part, other_part, term, total, send_out, recv_out,
    load_sem, gather_send, gather_recv, orb_send, orb_recv,
    small_send, small_recv, part_send, part_recv, out_send, out_recv, store_sem,
):
    walk, place = lax.axis_index("walk"), lax.axis_index("chol")
    x, z = lax.rem(walk, NX), lax.div(walk, NX)
    core, y = lax.rem(place, 2), lax.div(place, 2)

    def at_y(step):
        return lax.rem(y + step + NY, NY)

    def chol_of(step):
        return at_y(step) * 2 + core

    def on_x(step):
        return {"walk": z * NX + lax.rem(x + step + NX, NX), "chol": place}

    def on_z(step):
        return {"walk": lax.rem(z + step + NZ, NZ) * NX + x, "chol": place}

    def on_y(step):
        return {"walk": walk, "chol": chol_of(step)}

    partner = {"walk": walk, "chol": y * 2 + (1 - core)}

    barrier = pltpu.get_barrier_semaphore()

    def greet_walk(step, carry):
        pl.semaphore_signal(
            barrier, inc=1,
            device_id={"walk": lax.rem(walk + step, WALK), "chol": place}, device_id_type=MESH,
        )
        return carry

    def greet_chol(step, carry):
        pl.semaphore_signal(
            barrier, inc=1,
            device_id={"walk": walk, "chol": lax.rem(place + step, CHOL)}, device_id_type=MESH,
        )
        return carry

    lax.fori_loop(1, WALK, greet_walk, 0)
    lax.fori_loop(1, CHOL, greet_chol, 0)
    loads = [
        pltpu.make_async_copy(orb_in.at[0], orb.at[place], load_sem.at[0]),
        pltpu.make_async_copy(interp_in, ip.at[y], load_sem.at[1]),
        pltpu.make_async_copy(inv_in.at[0], inv, load_sem.at[2]),
        pltpu.make_async_copy(occ_in, occ, load_sem.at[3]),
        pltpu.make_async_copy(chol_in, chol, load_sem.at[4]),
        pltpu.make_async_copy(fields_in, fields, load_sem.at[5]),
    ]
    for load in loads:
        load.start()
    loads[2].wait()
    loads[3].wait()
    gathered[...] = lax.dot_general(
        inv[...], occ[...], (((0,), (0,)), ((), ())), preferred_element_type=F32
    )
    loads[0].wait()
    loads[1].wait()

    def turn(block, first, count):
        points = pl.ds(pl.multiple_of(block * PTS, PTS), PTS)
        for start in range(first, first + count, TURN):
            rows = slice(start, min(start + TURN, first + count))
            turned[points, rows] = ip[block, rows, :].T

    turn(y, 0, BASIS)
    loads[4].wait()
    loads[5].wait()
    pl.semaphore_wait(barrier, WALK - 1 + CHOL - 1)

    def moved(index, block, start, count, device):
        place_of = ip.at[block, pl.ds(pl.multiple_of(start, 16), count)]
        return pltpu.make_async_remote_copy(
            src_ref=place_of, dst_ref=place_of,
            send_sem=gather_send.at[index], recv_sem=gather_recv.at[index],
            device_id=device, device_id_type=MESH,
        )

    transfers = {}

    def start_gather(name, *what):
        copy = moved(len(transfers), *what)
        transfers[name] = copy
        copy.start()

    def landed(*names):
        for name in names:
            transfers[name].wait_recv()

    def x_piece(step):
        return lax.rem(x + step + NX, NX) * XROWS

    def z_piece(step):
        return ZBASE + lax.rem(z + step + NZ, NZ) * ZROWS

    def half_of(start, rows, half, way):
        return (start, half) if way == 1 else (start + half, rows - half)

    def x_half(step, way):
        return half_of(x_piece(step), XROWS, XHALF, way)

    def z_half(step, way):
        return half_of(z_piece(step), ZROWS, ZHALF, way)

    def c_half(way):
        return half_of(CBASE, CROWS, CHALF, way)

    def y0z():
        for way in (1, -1):
            start_gather(("y0z", way), y, z_piece(0), ZROWS, on_y(way))

    def y0x(first):
        for way in (1, -1):
            start_gather(("y0x", first, way), y, *x_half(0, way * first), on_y(way))

    def y0c(first):
        for way in (1, -1):
            start_gather(("y0c", first, way), y, *c_half(way * first), on_y(way))

    def y1z():
        for way in (1, -1):
            start_gather(("y1z", way), at_y(-way), *z_half(0, way), on_y(way))

    def y1x():
        for way in (1, -1):
            start_gather(("y1x", way), at_y(-way), *x_half(0, way), on_y(way))

    def y1c():
        for way in (1, -1):
            start_gather(("y1c", way), at_y(-way), *c_half(way), on_y(way))

    def x0(block, half):
        for way in (half, -half):
            start_gather(("x0", block, half, way), at_y(block), *x_half(0, half), on_x(way))

    def x1(block):
        for way in (1, -1):
            start_gather(("x1", block, way), at_y(block), *x_half(-way, way), on_x(way))

    def zs(step, block):
        for way in (1, -1):
            start_gather(
                (f"z{step}", block, way), at_y(block), z_piece(-way * step), ZROWS, on_z(way)
            )

    def z3(block):
        for way in (1, -1):
            start_gather(("z3", block, way), at_y(block), *z_half(-3 * way, way), on_z(way))

    def both(*stage):
        landed((*stage, 1), (*stage, -1))

    def orb_copy(index, block, rows, device):
        place_of = orb.at[block, rows]
        return pltpu.make_async_remote_copy(
            src_ref=place_of, dst_ref=place_of,
            send_sem=orb_send.at[index], recv_sem=orb_recv.at[index],
            device_id=device, device_id_type=MESH,
        )

    everything, lower, upper = pl.ds(0, ROWS), pl.ds(0, 208), pl.ds(208, 192)
    o_up = orb_copy(0, place, everything, on_y(1))
    o_down = orb_copy(1, place, everything, on_y(-1))
    o_across = orb_copy(2, place, everything, partner)
    o_up.start()
    o_down.start()
    o_across.start()
    y0z()

    def other(block):
        return lax.div(block, 2) * 2 + (1 - lax.rem(block, 2))

    def add_product(block, first=False):
        part = dot(orb[block], ip[y, pl.ds(pl.multiple_of(block * COLS, COLS), COLS), :])
        product[...] = part if first else product[...] + part

    below, above, far = chol_of(-1), chol_of(1), chol_of(2)
    add_product(place, True)
    o_up.wait_recv()
    o_up2 = orb_copy(3, below, lower, on_y(1))
    o_up2.start()
    o_across_below = orb_copy(4, below, everything, partner)
    o_across_below.start()
    o_down.wait_recv()
    o_down2 = orb_copy(5, above, upper, on_y(-1))
    o_down2.start()
    o_across_above = orb_copy(6, above, everything, partner)
    o_across_above.start()
    y0x(1)
    o_across.wait_recv()
    add_product(other(place))
    add_product(below)
    add_product(above)
    both("y0z")
    zs(0, -1)
    zs(0, 1)
    y1z()
    y0x(-1)
    o_across_below.wait_recv()
    add_product(other(below))
    o_across_above.wait_recv()
    add_product(other(above))
    o_up2.wait_recv()
    o_down2.wait_recv()
    o_across_far = orb_copy(7, far, everything, partner)
    o_across_far.start()
    add_product(far)
    o_across_far.wait_recv()
    add_product(other(far))

    weights[walk] = jnp.sum(gathered[...] * product[...], axis=0, keepdims=True)

    def send_weights(step, carry):
        pltpu.make_async_remote_copy(
            src_ref=weights.at[walk], dst_ref=weights.at[walk],
            send_sem=small_send.at[0], recv_sem=small_recv.at[0],
            device_id={"walk": lax.rem(walk + step, WALK), "chol": place}, device_id_type=MESH,
        ).start()
        return carry

    lax.fori_loop(1, WALK, send_weights, 0)
    both("y0x", 1)
    x0(-1, 1)
    x0(1, -1)
    both("y1z")
    zs(0, 2)
    both("z0", -1)
    zs(1, -1)
    both("y0x", -1)
    x0(-1, -1)
    x0(1, 1)
    y1x()
    y0c(1)
    both("z0", 1)
    zs(1, 1)
    window = pl.ds(pl.multiple_of(y * STEP, 16), WIN)
    for block in range(CHOL):
        rows = orb[block, window, :]
        term[:, block * COLS : (block + 1) * COLS] = rows
        total[:, block * COLS : (block + 1) * COLS] = rows.astype(F32)

    def multiply(block):
        current[block] = dot(term[...], ip[block])

    multiply(y)
    some = weights.at[pl.ds(0, WALK - 1)]
    pltpu.make_async_copy(some, some, small_recv.at[0]).wait()

    all_weights = weights[...].reshape(WALK, PTS)
    partial = sum_of_parts(dot(three_parts(all_weights), chol[...]), WALK)
    pair[core] = partial
    across = pltpu.make_async_remote_copy(
        src_ref=pair.at[core], dst_ref=pair.at[core],
        send_sem=small_send.at[4], recv_sem=small_recv.at[4],
        device_id=partner, device_id_type=MESH,
    )
    across.start()
    both("z0", 2)
    zs(1, 2)
    across.wait_recv()
    bias_parts[y] = pair[0] + pair[1]
    for step in (2, 1, 3):
        pltpu.make_async_remote_copy(
            src_ref=bias_parts.at[y], dst_ref=bias_parts.at[y],
            send_sem=small_send.at[1], recv_sem=small_recv.at[1],
            device_id=on_y(step), device_id_type=MESH,
        ).start()
    both("y1x")
    x0(2, 1)
    x0(2, -1)
    both("z1", -1)
    zs(2, -1)
    both("z1", 1)
    zs(2, 1)
    y0c(-1)
    some_bias = bias_parts.at[pl.ds(0, NY - 1)]
    pltpu.make_async_copy(some_bias, some_bias, small_recv.at[1]).wait()
    bias[...] = (bias_parts[0] + bias_parts[1]) + (bias_parts[2] + bias_parts[3])
    store_bias = pltpu.make_async_copy(bias, bias_out, store_sem.at[0])
    store_bias.start()

    coeff = TIME_ROOT * (fields[...] - bias[...])
    part = sum_of_parts(dot_last(three_parts(coeff), chol[...]), WALK)
    field_part[...] = part.reshape(WALK, 1, PTS)

    def send_scales(step, carry):
        to = lax.rem(walk + step, WALK)
        pltpu.make_async_remote_copy(
            src_ref=field_part.at[to], dst_ref=scale_in.at[walk],
            send_sem=small_send.at[2], recv_sem=small_recv.at[2],
            device_id={"walk": to, "chol": place}, device_id_type=MESH,
        ).start()
        return carry

    lax.fori_loop(1, WALK, send_scales, 0)
    scale_in[walk] = field_part[walk]
    both("z1", 2)
    zs(2, 2)
    for half in (1, -1):
        both("x0", -1, half)
        both("x0", 1, half)
    x1(-1)
    x1(1)
    both("y0c", 1)
    y1c()
    both("z2", -1)
    z3(-1)
    both("z2", 1)
    z3(1)
    some_scales = scale_in.at[pl.ds(0, WALK - 1)]
    pltpu.make_async_copy(some_scales, some_scales, small_recv.at[2]).wait()
    scales[y] = jnp.sum(scale_in[...], axis=0)
    to_up = [
        pltpu.make_async_remote_copy(
            src_ref=scales.at[y], dst_ref=scales.at[y],
            send_sem=small_send.at[3], recv_sem=small_recv.at[3],
            device_id=on_y(step), device_id_type=MESH,
        )
        for step in range(1, NY)
    ]
    for copy in to_up:
        copy.start()

    both("z2", 2)
    z3(2)
    both("x0", 2, 1)
    both("x0", 2, -1)
    x1(2)
    both("x1", -1)
    both("x1", 1)
    both("z3", -1)
    both("z3", 1)
    both("y0c", -1)
    for step in (-1, 1):
        turn(at_y(step), 0, BASIS)
        multiply(at_y(step))
    both("x1", 2)
    turn(at_y(2), 0, ZBASE)
    both("y1c")
    turn(at_y(2), CBASE, CROWS)
    both("z3", 2)
    turn(at_y(2), ZBASE, CBASE - ZBASE)
    multiply(at_y(2))
    some_blocks = scales.at[pl.ds(0, NY - 1)]
    pltpu.make_async_copy(some_blocks, some_blocks, small_recv.at[3]).wait()

    def exchange(slot, tile):
        return pltpu.make_async_remote_copy(
            src_ref=own_part.at[slot, tile], dst_ref=other_part.at[slot, tile],
            send_sem=part_send.at[slot, tile], recv_sem=part_recv.at[slot, tile],
            device_id=partner, device_id_type=MESH,
        )

    def points_to_basis(slot):
        for block in range(NY):
            mixed[:, block * PTS : (block + 1) * PTS] = (
                current[block] * (scales[block] / (slot + 1).astype(F32))
            ).astype(BF16)

        for tile in range(TILES):
            columns = slice(tile * TILE, (tile + 1) * TILE)
            own_part[slot, tile] = dot(mixed[...], turned[:, columns]).astype(BF16)
            exchange(slot, tile).start()

    def summed(slot, tile):
        exchange(slot, tile).wait_recv()
        columns = slice(tile * TILE, (tile + 1) * TILE)
        value = (own_part[slot, tile].astype(F32) + other_part[slot, tile].astype(F32)).astype(BF16)
        total[:, columns] = total[:, columns] + value.astype(F32)
        return value

    def one_term(slot, carry):
        points_to_basis(slot)
        for tile in range(TILES):
            value = summed(slot, tile)
            for block in range(NY):
                part = dot(value, ip[block, tile * TILE : (tile + 1) * TILE, :])
                current[block] = current[block] + part if tile else part
        return carry

    lax.fori_loop(0, TERMS - 1, one_term, 0)
    points_to_basis(jnp.int32(TERMS - 1))
    for tile in range(TILES):
        summed(TERMS - 1, tile)

    for step in (2, 1, 3, 0):
        to = at_y(step)
        columns = pl.ds(pl.multiple_of((to * 2 + core) * COLS, COLS), COLS)
        send_out[to] = total[:, columns].astype(BF16)
        if step:
            pltpu.make_async_remote_copy(
                src_ref=send_out.at[to], dst_ref=recv_out.at[y],
                send_sem=out_send, recv_sem=out_recv,
                device_id=on_y(step), device_id_type=MESH,
            ).start()
    recv_out[y] = send_out[y]
    for copy in transfers.values():
        copy.wait_send()
    for copy in (o_up, o_down, o_across, o_up2, o_down2, o_across_below, o_across_above, o_across_far):
        copy.wait_send()
    pltpu.make_async_copy(some, some, small_send.at[0]).wait()
    pltpu.make_async_copy(some_bias, some_bias, small_send.at[1]).wait()
    pltpu.make_async_copy(some_scales, some_scales, small_send.at[2]).wait()
    pltpu.make_async_copy(some_blocks, some_blocks, small_send.at[3]).wait()
    across.wait_send()
    for slot in range(TERMS):
        for tile in range(TILES):
            pltpu.make_async_copy(
                own_part.at[slot, tile], other_part.at[slot, tile], part_send.at[slot, tile]
            ).wait()
    some_out = recv_out.at[pl.ds(0, NY - 1)]
    pltpu.make_async_copy(some_out, some_out, out_recv).wait()
    stores = []
    for part in range(NY):
        count = WIN if part == NY - 1 else STEP
        stores.append(
            pltpu.make_async_copy(
                recv_out.at[part, pl.ds(0, count)], out.at[0, pl.ds(part * STEP, count)],
                store_sem.at[1 + part],
            )
        )
    for store in stores:
        store.start()

    pltpu.make_async_copy(some_out, some_out, out_send).wait()
    store_bias.wait()
    for store in stores:
        store.wait()


N_GATHER = 16 + 18 + 24


def on_device(orbitals, intersection_inv, interp, occ_interp, chol_factors, fields):
    dma = pltpu.SemaphoreType.DMA
    hbm = pl.BlockSpec(memory_space=pl.ANY)
    return pl.pallas_call(
        kernel,
        out_shape=(
            jax.ShapeDtypeStruct((1, ROWS, COLS), BF16),
            jax.ShapeDtypeStruct((WALK, VEC), F32),
        ),
        in_specs=[hbm] * 6,
        out_specs=(hbm, hbm),
        scratch_shapes=[
            pltpu.VMEM((NY, BASIS, PTS), BF16),
            pltpu.VMEM((NY * PTS, BASIS), BF16),
            pltpu.VMEM((CHOL, ROWS, COLS), BF16),
            pltpu.VMEM((ROWS, ROWS), BF16),
            pltpu.VMEM((ROWS, PTS), BF16),
            pltpu.VMEM((PTS, VEC), BF16),
            pltpu.VMEM((WALK, VEC), F32),
            pltpu.VMEM((ROWS, PTS), F32),
            pltpu.VMEM((ROWS, PTS), F32),
            pltpu.VMEM((WALK, 1, PTS), F32),
            pltpu.VMEM((2, WALK, VEC), F32),
            pltpu.VMEM((NY, WALK, VEC), F32),
            pltpu.VMEM((WALK, VEC), F32),
            pltpu.VMEM((WALK, 1, PTS), F32),
            pltpu.VMEM((WALK, 1, PTS), F32),
            pltpu.VMEM((NY, 1, PTS), F32),
            pltpu.VMEM((NY, WIN, PTS), F32),
            pltpu.VMEM((WIN, NY * PTS), BF16),
            pltpu.VMEM((TERMS, TILES, WIN, TILE), BF16),
            pltpu.VMEM((TERMS, TILES, WIN, TILE), BF16),
            pltpu.VMEM((WIN, BASIS), BF16),
            pltpu.VMEM((WIN, BASIS), F32),
            pltpu.VMEM((NY, WIN, COLS), BF16),
            pltpu.VMEM((NY, WIN, COLS), BF16),
            dma((6,)),
            dma((N_GATHER,)),
            dma((N_GATHER,)),
            dma((8,)),
            dma((8,)),
            dma((5,)),
            dma((5,)),
            dma((TERMS, TILES)),
            dma((TERMS, TILES)),
            dma,
            dma,
            dma((5,)),
        ],
        compiler_params=pltpu.CompilerParams(
            collective_id=0, has_side_effects=True, vmem_limit_bytes=60 * 1024 * 1024
        ),
    )(orbitals, intersection_inv, interp, occ_interp, chol_factors, fields)


def solution(mesh):
    placed = (
        P("walk", None, "chol"),
        P("walk", None, None),
        P(None, "chol"),
        P(None, "chol"),
        P("chol", "walk"),
        P(None, "walk"),
    )
    return jax.shard_map(
        on_device,
        mesh=mesh,
        in_specs=placed,
        out_specs=(P("walk", None, "chol"), P(None, "walk")),
        check_vma=False,
    )
```

```python
import jax
import jax.numpy as jnp
from jax import lax
from jax.experimental import pallas as pl
from jax.experimental.pallas import tpu as pltpu
from jax.sharding import PartitionSpec as P

TERMS = 4
TIME_ROOT = 2.2
MESH = pl.DeviceIdType.MESH
F32, BF16 = jnp.float32, jnp.bfloat16

NX, NZ, NY = 4, 8, 4
WALK, CHOL = NX * NZ, NY * 2
ROWS, BASIS, PTS, VEC = 400, 2048, 512, 256
COLS = BASIS // CHOL
WIN, STEP = 112, 96
XROWS, XHALF = 192, 96
ZROWS, ZHALF = 112, 64
ZBASE = NX * XROWS
CBASE = ZBASE + NZ * ZROWS
CROWS, CHALF = BASIS - CBASE, 192
TILE = 512
TILES = BASIS // TILE
TURN = 512


def three_parts(value):
    high = value.astype(BF16)
    rest = value - high.astype(F32)
    middle = rest.astype(BF16)
    low = (rest - middle.astype(F32)).astype(BF16)
    return jnp.concatenate([high, middle, low], axis=0)


def sum_of_parts(value, rows):
    return value[:rows] + value[rows : 2 * rows] + value[2 * rows :]


def dot(left, right):
    return jnp.dot(left, right, preferred_element_type=F32)


def dot_last(left, right):
    return lax.dot_general(left, right, (((1,), (1,)), ((), ())), preferred_element_type=F32)


def kernel(
    orb_in, inv_in, interp_in, occ_in, chol_in, fields_in,
    recv_out, bias,
    ip, turned, orb, inv, occ, chol, fields,
    gathered, product, weights, pair, bias_parts, field_part, scale_in, scales,
    current, mixed, own_part, other_part, term, total, send_out,
    load_sem, gather_send, gather_recv, orb_send, orb_recv,
    small_send, small_recv, part_send, part_recv, out_send, out_recv,
):
    walk, place = lax.axis_index("walk"), lax.axis_index("chol")
    x, z = lax.rem(walk, NX), lax.div(walk, NX)
    core, y = lax.rem(place, 2), lax.div(place, 2)

    def at_y(step):
        return lax.rem(y + step + NY, NY)

    def chol_of(step):
        return at_y(step) * 2 + core

    def on_x(step):
        return {"walk": z * NX + lax.rem(x + step + NX, NX), "chol": place}

    def on_z(step):
        return {"walk": lax.rem(z + step + NZ, NZ) * NX + x, "chol": place}

    def on_y(step):
        return {"walk": walk, "chol": chol_of(step)}

    partner = {"walk": walk, "chol": y * 2 + (1 - core)}

    barrier = pltpu.get_barrier_semaphore()

    def greet_walk(step, carry):
        pl.semaphore_signal(
            barrier, inc=1,
            device_id={"walk": lax.rem(walk + step, WALK), "chol": place}, device_id_type=MESH,
        )
        return carry

    def greet_chol(step, carry):
        pl.semaphore_signal(
            barrier, inc=1,
            device_id={"walk": walk, "chol": lax.rem(place + step, CHOL)}, device_id_type=MESH,
        )
        return carry

    lax.fori_loop(1, WALK, greet_walk, 0)
    lax.fori_loop(1, CHOL, greet_chol, 0)
    loads = [
        pltpu.make_async_copy(orb_in.at[0], orb.at[place], load_sem.at[0]),
        pltpu.make_async_copy(interp_in, ip.at[y], load_sem.at[1]),
        pltpu.make_async_copy(inv_in.at[0], inv, load_sem.at[2]),
        pltpu.make_async_copy(occ_in, occ, load_sem.at[3]),
        pltpu.make_async_copy(chol_in, chol, load_sem.at[4]),
        pltpu.make_async_copy(fields_in, fields, load_sem.at[5]),
    ]
    for load in loads:
        load.start()
    def turn(block, first, count):
        points = pl.ds(pl.multiple_of(block * PTS, PTS), PTS)
        for start in range(first, first + count, TURN):
            rows = slice(start, min(start + TURN, first + count))
            turned[points, rows] = ip[block, rows, :].T

    loads[0].wait()
    loads[1].wait()
    pl.semaphore_wait(barrier, WALK - 1 + CHOL - 1)

    def moved(index, block, start, count, device):
        place_of = ip.at[block, pl.ds(pl.multiple_of(start, 16), count)]
        return pltpu.make_async_remote_copy(
            src_ref=place_of, dst_ref=place_of,
            send_sem=gather_send.at[index], recv_sem=gather_recv.at[index],
            device_id=device, device_id_type=MESH,
        )

    transfers = {}

    def start_gather(name, *what):
        copy = moved(len(transfers), *what)
        transfers[name] = copy
        copy.start()

    def landed(*names):
        for name in names:
            transfers[name].wait_recv()

    def x_piece(step):
        return lax.rem(x + step + NX, NX) * XROWS

    def z_piece(step):
        return ZBASE + lax.rem(z + step + NZ, NZ) * ZROWS

    def half_of(start, rows, half, way):
        return (start, half) if way == 1 else (start + half, rows - half)

    def x_half(step, way):
        return half_of(x_piece(step), XROWS, XHALF, way)

    def z_half(step, way):
        return half_of(z_piece(step), ZROWS, ZHALF, way)

    def c_half(way):
        return half_of(CBASE, CROWS, CHALF, way)

    def y0z():
        for way in (1, -1):
            start_gather(("y0z", way), y, z_piece(0), ZROWS, on_y(way))

    def y0x(first):
        for way in (1, -1):
            start_gather(("y0x", first, way), y, *x_half(0, way * first), on_y(way))

    def y0c(first):
        for way in (1, -1):
            start_gather(("y0c", first, way), y, *c_half(way * first), on_y(way))

    def y1z():
        for way in (1, -1):
            start_gather(("y1z", way), at_y(-way), *z_half(0, way), on_y(way))

    def y1x():
        for way in (1, -1):
            start_gather(("y1x", way), at_y(-way), *x_half(0, way), on_y(way))

    def y1c():
        for way in (1, -1):
            start_gather(("y1c", way), at_y(-way), *c_half(way), on_y(way))

    def x0(block, half):
        for way in (half, -half):
            start_gather(("x0", block, half, way), at_y(block), *x_half(0, half), on_x(way))

    def x1(block):
        for way in (1, -1):
            start_gather(("x1", block, way), at_y(block), *x_half(-way, way), on_x(way))

    def zs(step, block):
        for way in (1, -1):
            start_gather(
                (f"z{step}", block, way), at_y(block), z_piece(-way * step), ZROWS, on_z(way)
            )

    def z3(block):
        for way in (1, -1):
            start_gather(("z3", block, way), at_y(block), *z_half(-3 * way, way), on_z(way))

    def both(*stage):
        landed((*stage, 1), (*stage, -1))

    def orb_copy(index, block, rows, device):
        place_of = orb.at[block, rows]
        return pltpu.make_async_remote_copy(
            src_ref=place_of, dst_ref=place_of,
            send_sem=orb_send.at[index], recv_sem=orb_recv.at[index],
            device_id=device, device_id_type=MESH,
        )

    everything, lower, upper = pl.ds(0, ROWS), pl.ds(0, 208), pl.ds(208, 192)
    below, above, far = chol_of(-1), chol_of(1), chol_of(2)
    o_up = [orb_copy(0, place, lower, on_y(1)), orb_copy(1, place, upper, on_y(1))]
    o_down = [orb_copy(2, place, upper, on_y(-1)), orb_copy(3, place, lower, on_y(-1))]
    o_across = orb_copy(4, place, everything, partner)
    y0z()
    for copy in (o_up[0], o_down[0], o_up[1], o_down[1], o_across):
        copy.start()

    def other(block):
        return lax.div(block, 2) * 2 + (1 - lax.rem(block, 2))

    def add_product(block, first=False):
        part = dot(orb[block], ip[y, pl.ds(pl.multiple_of(block * COLS, COLS), COLS), :])
        product[...] = part if first else product[...] + part

    for load in loads[2:]:
        load.wait()
    gathered[...] = lax.dot_general(
        inv[...], occ[...], (((0,), (0,)), ((), ())), preferred_element_type=F32
    )
    add_product(place, True)
    both("y0z")
    zs(0, -1)
    zs(0, 1)
    o_up[0].wait_recv()
    o_up2 = orb_copy(5, below, lower, on_y(1))
    o_up2.start()
    o_down[0].wait_recv()
    o_down2 = orb_copy(6, above, upper, on_y(-1))
    o_down2.start()
    y1z()
    y0x(1)
    turn(y, 0, BASIS)
    o_up[1].wait_recv()
    o_across_below = orb_copy(7, below, everything, partner)
    o_across_below.start()
    o_down[1].wait_recv()
    o_across_above = orb_copy(8, above, everything, partner)
    o_across_above.start()
    o_across.wait_recv()
    add_product(other(place))
    both("z0", -1)
    zs(1, -1)
    add_product(below)
    add_product(above)
    o_across_below.wait_recv()
    add_product(other(below))
    o_across_above.wait_recv()
    add_product(other(above))
    o_up2.wait_recv()
    o_down2.wait_recv()
    o_across_far = orb_copy(9, far, everything, partner)
    o_across_far.start()
    both("z0", 1)
    zs(1, 1)
    add_product(far)
    y0x(-1)
    o_across_far.wait_recv()
    add_product(other(far))

    weights[walk] = jnp.sum(gathered[...] * product[...], axis=0, keepdims=True)

    def send_weights(step, carry):
        pltpu.make_async_remote_copy(
            src_ref=weights.at[walk], dst_ref=weights.at[walk],
            send_sem=small_send.at[0], recv_sem=small_recv.at[0],
            device_id={"walk": lax.rem(walk + step, WALK), "chol": place}, device_id_type=MESH,
        ).start()
        return carry

    lax.fori_loop(1, WALK, send_weights, 0)
    both("y1z")
    zs(0, 2)
    both("y0x", 1)
    x0(-1, 1)
    x0(1, -1)
    both("z1", -1)
    zs(2, -1)
    both("z1", 1)
    zs(2, 1)
    both("y0x", -1)
    x0(-1, -1)
    x0(1, 1)
    y1x()
    y0c(1)
    window = pl.ds(pl.multiple_of(y * STEP, 16), WIN)
    for block in range(CHOL):
        rows = orb[block, window, :]
        term[:, block * COLS : (block + 1) * COLS] = rows
        total[:, block * COLS : (block + 1) * COLS] = rows.astype(F32)

    def multiply(block):
        current[block] = dot(term[...], ip[block])

    multiply(y)
    some = weights.at[pl.ds(0, WALK - 1)]
    pltpu.make_async_copy(some, some, small_recv.at[0]).wait()

    all_weights = weights[...].reshape(WALK, PTS)
    partial = sum_of_parts(dot(three_parts(all_weights), chol[...]), WALK)
    pair[core] = partial
    across = pltpu.make_async_remote_copy(
        src_ref=pair.at[core], dst_ref=pair.at[core],
        send_sem=small_send.at[4], recv_sem=small_recv.at[4],
        device_id=partner, device_id_type=MESH,
    )
    across.start()
    both("z0", 2)
    zs(1, 2)
    across.wait_recv()
    bias_parts[y] = pair[0] + pair[1]
    for step in (2, 1, 3):
        pltpu.make_async_remote_copy(
            src_ref=bias_parts.at[y], dst_ref=bias_parts.at[y],
            send_sem=small_send.at[1], recv_sem=small_recv.at[1],
            device_id=on_y(step), device_id_type=MESH,
        ).start()
    both("y1x")
    x0(2, 1)
    x0(2, -1)
    both("z2", -1)
    z3(-1)
    both("z2", 1)
    z3(1)
    y0c(-1)
    some_bias = bias_parts.at[pl.ds(0, NY - 1)]
    pltpu.make_async_copy(some_bias, some_bias, small_recv.at[1]).wait()
    bias[...] = (bias_parts[0] + bias_parts[1]) + (bias_parts[2] + bias_parts[3])

    coeff = TIME_ROOT * (fields[...] - bias[...])
    part = sum_of_parts(dot_last(three_parts(coeff), chol[...]), WALK)
    field_part[...] = part.reshape(WALK, 1, PTS)

    def send_scales(step, carry):
        to = lax.rem(walk + step, WALK)
        pltpu.make_async_remote_copy(
            src_ref=field_part.at[to], dst_ref=scale_in.at[walk],
            send_sem=small_send.at[2], recv_sem=small_recv.at[2],
            device_id={"walk": to, "chol": place}, device_id_type=MESH,
        ).start()
        return carry

    lax.fori_loop(1, WALK, send_scales, 0)
    scale_in[walk] = field_part[walk]
    both("z1", 2)
    zs(2, 2)
    for half in (1, -1):
        both("x0", -1, half)
        both("x0", 1, half)
    x1(-1)
    x1(1)
    both("y0c", 1)
    y1c()
    both("x0", 2, 1)
    both("x0", 2, -1)
    x1(2)
    both("z3", -1)
    both("z3", 1)
    for step in (-1, 1):
        turn(at_y(step), ZBASE, CBASE - ZBASE)
    both("z2", 2)
    z3(2)
    both("y0c", -1)
    for step in (-1, 1):
        turn(at_y(step), CBASE, CROWS)
    some_scales = scale_in.at[pl.ds(0, WALK - 1)]
    pltpu.make_async_copy(some_scales, some_scales, small_recv.at[2]).wait()
    scales[y] = jnp.sum(scale_in[...], axis=0)
    to_up = [
        pltpu.make_async_remote_copy(
            src_ref=scales.at[y], dst_ref=scales.at[y],
            send_sem=small_send.at[3], recv_sem=small_recv.at[3],
            device_id=on_y(step), device_id_type=MESH,
        )
        for step in range(1, NY)
    ]
    for copy in to_up:
        copy.start()

    both("x1", -1)
    both("x1", 1)
    for step in (-1, 1):
        turn(at_y(step), 0, ZBASE)
        multiply(at_y(step))
    both("y1c")
    both("z3", 2)
    turn(at_y(2), ZBASE, BASIS - ZBASE)
    both("x1", 2)
    turn(at_y(2), 0, ZBASE)
    multiply(at_y(2))
    some_blocks = scales.at[pl.ds(0, NY - 1)]
    pltpu.make_async_copy(some_blocks, some_blocks, small_recv.at[3]).wait()

    def exchange(slot, tile):
        return pltpu.make_async_remote_copy(
            src_ref=own_part.at[slot, tile], dst_ref=other_part.at[slot, tile],
            send_sem=part_send.at[slot, tile], recv_sem=part_recv.at[slot, tile],
            device_id=partner, device_id_type=MESH,
        )

    def mix(slot):
        for block in range(NY):
            mixed[:, block * PTS : (block + 1) * PTS] = (
                current[block] * (scales[block] / (slot + 1).astype(F32))
            ).astype(BF16)

    def points_to_basis(slot):
        mix(slot)
        for tile in range(TILES):
            columns = slice(tile * TILE, (tile + 1) * TILE)
            own_part[slot, tile] = dot(mixed[...], turned[:, columns]).astype(BF16)
            exchange(slot, tile).start()

    def summed(slot, tile):
        exchange(slot, tile).wait_recv()
        columns = slice(tile * TILE, (tile + 1) * TILE)
        value = (own_part[slot, tile].astype(F32) + other_part[slot, tile].astype(F32)).astype(BF16)
        total[:, columns] = total[:, columns] + value.astype(F32)
        return value

    def one_term(slot, carry):
        points_to_basis(slot)
        for tile in range(TILES):
            value = summed(slot, tile)
            for block in range(NY):
                part = dot(value, ip[block, tile * TILE : (tile + 1) * TILE, :])
                current[block] = current[block] + part if tile else part
        return carry

    lax.fori_loop(0, TERMS - 1, one_term, 0)
    last = TERMS - 1
    mix(jnp.int32(last))
    mine = pl.ds(pl.multiple_of(core * COLS, COLS), COLS)
    others = pl.ds(pl.multiple_of((1 - core) * COLS, COLS), COLS)

    def exchange_half(tile):
        return pltpu.make_async_remote_copy(
            src_ref=own_part.at[last, tile, :, others], dst_ref=other_part.at[last, tile, :, others],
            send_sem=part_send.at[last, tile], recv_sem=part_recv.at[last, tile],
            device_id=partner, device_id_type=MESH,
        )

    def begin(step):
        to = at_y(step)
        columns = pl.ds(pl.multiple_of(to * TILE, TILE), TILE)
        own_part[last, to] = dot(mixed[...], turned[:, columns]).astype(BF16)
        exchange_half(to).start()

    def finish(step):
        to = at_y(step)
        exchange_half(to).wait_recv()
        value = own_part[last, to, :, mine].astype(F32) + other_part[last, to, :, mine].astype(F32)
        columns = pl.ds(pl.multiple_of(to * TILE + core * COLS, COLS), COLS)
        row = (total[:, columns] + value.astype(BF16).astype(F32)).astype(BF16)
        if step:
            send_out[to] = row
            pltpu.make_async_remote_copy(
                src_ref=send_out.at[to], dst_ref=recv_out.at[y],
                send_sem=out_send, recv_sem=out_recv,
                device_id=on_y(step), device_id_type=MESH,
            ).start()
        else:
            recv_out[y] = row

    begin(2)
    begin(1)
    begin(3)
    finish(2)
    finish(1)
    begin(0)
    finish(3)
    finish(0)
    for copy in transfers.values():
        copy.wait_send()
    for copy in (*o_up, *o_down, o_across, o_up2, o_down2, o_across_below, o_across_above, o_across_far):
        copy.wait_send()
    pltpu.make_async_copy(some, some, small_send.at[0]).wait()
    pltpu.make_async_copy(some_bias, some_bias, small_send.at[1]).wait()
    pltpu.make_async_copy(some_scales, some_scales, small_send.at[2]).wait()
    pltpu.make_async_copy(some_blocks, some_blocks, small_send.at[3]).wait()
    across.wait_send()
    for slot in range(TERMS):
        for tile in range(TILES):
            (exchange if slot < last else lambda _, to: exchange_half(to))(slot, tile).wait_send()
    some_out = recv_out.at[pl.ds(0, NY - 1)]
    pltpu.make_async_copy(some_out, some_out, out_recv).wait()
    pltpu.make_async_copy(some_out, some_out, out_send).wait()


def assemble(parts, bias_in, out, bias_out):
    for part in range(NY):
        count = WIN if part == NY - 1 else STEP
        out[0, part * STEP : part * STEP + count] = parts[part, :count]
    bias_out[...] = bias_in[...]


N_GATHER = 16 + 18 + 24


def on_device(orbitals, intersection_inv, interp, occ_interp, chol_factors, fields):
    dma = pltpu.SemaphoreType.DMA
    hbm = pl.BlockSpec(memory_space=pltpu.HBM)
    vmem = pl.BlockSpec(memory_space=pltpu.VMEM)
    pieces = pl.pallas_call(
        kernel,
        out_shape=(
            jax.ShapeDtypeStruct((NY, WIN, COLS), BF16),
            jax.ShapeDtypeStruct((WALK, VEC), F32),
        ),
        in_specs=[hbm] * 6,
        out_specs=(vmem, vmem),
        scratch_shapes=[
            pltpu.VMEM((NY, BASIS, PTS), BF16),
            pltpu.VMEM((NY * PTS, BASIS), BF16),
            pltpu.VMEM((CHOL, ROWS, COLS), BF16),
            pltpu.VMEM((ROWS, ROWS), BF16),
            pltpu.VMEM((ROWS, PTS), BF16),
            pltpu.VMEM((PTS, VEC), BF16),
            pltpu.VMEM((WALK, VEC), F32),
            pltpu.VMEM((ROWS, PTS), F32),
            pltpu.VMEM((ROWS, PTS), F32),
            pltpu.VMEM((WALK, 1, PTS), F32),
            pltpu.VMEM((2, WALK, VEC), F32),
            pltpu.VMEM((NY, WALK, VEC), F32),
            pltpu.VMEM((WALK, 1, PTS), F32),
            pltpu.VMEM((WALK, 1, PTS), F32),
            pltpu.VMEM((NY, 1, PTS), F32),
            pltpu.VMEM((NY, WIN, PTS), F32),
            pltpu.VMEM((WIN, NY * PTS), BF16),
            pltpu.VMEM((TERMS, TILES, WIN, TILE), BF16),
            pltpu.VMEM((TERMS, TILES, WIN, TILE), BF16),
            pltpu.VMEM((WIN, BASIS), BF16),
            pltpu.VMEM((WIN, BASIS), F32),
            pltpu.VMEM((NY, WIN, COLS), BF16),
            dma((6,)),
            dma((N_GATHER,)),
            dma((N_GATHER,)),
            dma((10,)),
            dma((10,)),
            dma((5,)),
            dma((5,)),
            dma((TERMS, TILES)),
            dma((TERMS, TILES)),
            dma,
            dma,
        ],
        compiler_params=pltpu.CompilerParams(
            collective_id=0, has_side_effects=True, vmem_limit_bytes=44 * 1024 * 1024
        ),
    )(
        *(
            pltpu.with_memory_space_constraint(value, pltpu.HBM)
            for value in (orbitals, intersection_inv, interp, occ_interp, chol_factors, fields)
        )
    )
    return pl.pallas_call(
        assemble,
        out_shape=(
            jax.ShapeDtypeStruct((1, ROWS, COLS), BF16),
            jax.ShapeDtypeStruct((WALK, VEC), F32),
        ),
        in_specs=[vmem] * 2,
        out_specs=(vmem, vmem),
        compiler_params=pltpu.CompilerParams(vmem_limit_bytes=8 * 1024 * 1024),
    )(*pieces)


def solution(mesh):
    placed = (
        P("walk", None, "chol"),
        P("walk", None, None),
        P(None, "chol"),
        P(None, "chol"),
        P("chol", "walk"),
        P(None, "walk"),
    )
    return jax.shard_map(
        on_device,
        mesh=mesh,
        in_specs=placed,
        out_specs=(P("walk", None, "chol"), P(None, "walk")),
        check_vma=False,
    )
```

```python
import jax
import jax.numpy as jnp
from jax import lax
from jax.experimental import pallas as pl
from jax.experimental.pallas import tpu as pltpu
from jax.sharding import PartitionSpec as P

TERMS = 4
TIME_ROOT = 2.2
MESH = pl.DeviceIdType.MESH
F32, BF16 = jnp.float32, jnp.bfloat16

NX, NZ, NY = 4, 8, 4
WALK, CHOL = NX * NZ, NY * 2
ROWS, BASIS, PTS, VEC = 400, 2048, 512, 256
COLS = BASIS // CHOL
WIN, STEP = 112, 96
XROWS, XHALF = 192, 96
ZROWS, ZHALF = 112, 64
ZBASE = NX * XROWS
CBASE = ZBASE + NZ * ZROWS
CROWS, CHALF = BASIS - CBASE, 192
TILE = 512
TILES = BASIS // TILE
TURN = 512


def three_parts(value):
    high = value.astype(BF16)
    rest = value - high.astype(F32)
    middle = rest.astype(BF16)
    low = (rest - middle.astype(F32)).astype(BF16)
    return jnp.concatenate([high, middle, low], axis=0)


def sum_of_parts(value, rows):
    return value[:rows] + value[rows : 2 * rows] + value[2 * rows :]


def dot(left, right):
    return jnp.dot(left, right, preferred_element_type=F32)


def dot_last(left, right):
    return lax.dot_general(left, right, (((1,), (1,)), ((), ())), preferred_element_type=F32)


def kernel(
    orb_in, inv_in, interp_in, occ_in, chol_in, fields_in,
    recv_out, bias,
    ip, turned, orb, inv, occ, chol, fields,
    gathered, product, weights, pair, bias_parts, field_part, scale_in, scales,
    current, mixed, own_part, other_part, term, total, send_out,
    load_sem, gather_send, gather_recv, orb_send, orb_recv,
    small_send, small_recv, part_send, part_recv, out_send, out_recv, ready,
):
    walk, place = lax.axis_index("walk"), lax.axis_index("chol")
    x, z = lax.rem(walk, NX), lax.div(walk, NX)
    core, y = lax.rem(place, 2), lax.div(place, 2)

    def at_y(step):
        return lax.rem(y + step + NY, NY)

    def chol_of(step):
        return at_y(step) * 2 + core

    def on_x(step):
        return {"walk": z * NX + lax.rem(x + step + NX, NX), "chol": place}

    def on_z(step):
        return {"walk": lax.rem(z + step + NZ, NZ) * NX + x, "chol": place}

    def on_y(step):
        return {"walk": walk, "chol": chol_of(step)}

    partner = {"walk": walk, "chol": y * 2 + (1 - core)}

    barrier = pltpu.get_barrier_semaphore()

    loads = [
        pltpu.make_async_copy(orb_in.at[0], orb.at[place], load_sem.at[0]),
        pltpu.make_async_copy(interp_in, ip.at[y], load_sem.at[1]),
        pltpu.make_async_copy(inv_in.at[0], inv, load_sem.at[2]),
        pltpu.make_async_copy(occ_in, occ, load_sem.at[3]),
        pltpu.make_async_copy(chol_in, chol, load_sem.at[4]),
        pltpu.make_async_copy(fields_in, fields, load_sem.at[5]),
    ]
    for load in loads:
        load.start()
    neighbours = [on_x(1), on_x(-1), on_z(1), on_z(-1)]

    def greet(step, carry):
        pl.semaphore_signal(
            barrier, inc=1,
            device_id={"walk": walk, "chol": lax.rem(place + step, CHOL)}, device_id_type=MESH,
        )
        return carry

    for device in neighbours:
        pl.semaphore_signal(barrier, inc=1, device_id=device, device_id_type=MESH)
    lax.fori_loop(1, CHOL, greet, 0)

    def tell(index, devices):
        for device in devices:
            pl.semaphore_signal(ready.at[index], inc=1, device_id=device, device_id_type=MESH)

    def pass_on(index):
        pl.semaphore_wait(ready.at[index], 2)
        if index < NZ // 2:
            tell(index + 1, neighbours[2:])
    def turn(block, first, count):
        points = pl.ds(pl.multiple_of(block * PTS, PTS), PTS)
        for start in range(first, first + count, TURN):
            rows = slice(start, min(start + TURN, first + count))
            turned[points, rows] = ip[block, rows, :].T

    pl.semaphore_wait(barrier, CHOL - 1 + len(neighbours))
    loads[0].wait()
    loads[1].wait()

    def moved(index, block, start, count, device):
        place_of = ip.at[block, pl.ds(pl.multiple_of(start, 16), count)]
        return pltpu.make_async_remote_copy(
            src_ref=place_of, dst_ref=place_of,
            send_sem=gather_send.at[index], recv_sem=gather_recv.at[index],
            device_id=device, device_id_type=MESH,
        )

    transfers = {}

    def start_gather(name, *what):
        copy = moved(len(transfers), *what)
        transfers[name] = copy
        copy.start()

    def landed(*names):
        for name in names:
            transfers[name].wait_recv()

    def x_piece(step):
        return lax.rem(x + step + NX, NX) * XROWS

    def z_piece(step):
        return ZBASE + lax.rem(z + step + NZ, NZ) * ZROWS

    def half_of(start, rows, half, way):
        return (start, half) if way == 1 else (start + half, rows - half)

    def x_half(step, way):
        return half_of(x_piece(step), XROWS, XHALF, way)

    def z_half(step, way):
        return half_of(z_piece(step), ZROWS, ZHALF, way)

    def c_half(way):
        return half_of(CBASE, CROWS, CHALF, way)

    def y0z():
        for way in (1, -1):
            start_gather(("y0z", way), y, z_piece(0), ZROWS, on_y(way))

    def y0x(first):
        for way in (1, -1):
            start_gather(("y0x", first, way), y, *x_half(0, way * first), on_y(way))

    def y0c(first):
        for way in (1, -1):
            start_gather(("y0c", first, way), y, *c_half(way * first), on_y(way))

    def y1z():
        for way in (1, -1):
            start_gather(("y1z", way), at_y(-way), *z_half(0, way), on_y(way))

    def y1x():
        for way in (1, -1):
            start_gather(("y1x", way), at_y(-way), *x_half(0, way), on_y(way))

    def y1c():
        for way in (1, -1):
            start_gather(("y1c", way), at_y(-way), *c_half(way), on_y(way))

    def x0(block, half):
        for way in (half, -half):
            start_gather(("x0", block, half, way), at_y(block), *x_half(0, half), on_x(way))

    def x1(block):
        for way in (1, -1):
            start_gather(("x1", block, way), at_y(block), *x_half(-way, way), on_x(way))

    def zs(step, block):
        for way in (1, -1):
            start_gather(
                (f"z{step}", block, way), at_y(block), z_piece(-way * step), ZROWS, on_z(way)
            )

    def z3(block):
        for way in (1, -1):
            start_gather(("z3", block, way), at_y(block), *z_half(-3 * way, way), on_z(way))

    def both(*stage):
        landed((*stage, 1), (*stage, -1))

    def orb_copy(index, block, rows, device):
        place_of = orb.at[block, rows]
        return pltpu.make_async_remote_copy(
            src_ref=place_of, dst_ref=place_of,
            send_sem=orb_send.at[index], recv_sem=orb_recv.at[index],
            device_id=device, device_id_type=MESH,
        )

    everything, lower, upper = pl.ds(0, ROWS), pl.ds(0, 208), pl.ds(208, 192)
    below, above, far = chol_of(-1), chol_of(1), chol_of(2)
    o_up = [orb_copy(0, place, lower, on_y(1)), orb_copy(1, place, upper, on_y(1))]
    o_down = [orb_copy(2, place, upper, on_y(-1)), orb_copy(3, place, lower, on_y(-1))]
    o_across = orb_copy(4, place, everything, partner)
    y0z()
    for copy in (o_up[0], o_down[0], o_up[1], o_down[1], o_across):
        copy.start()
    tell(0, neighbours[:2])

    def other(block):
        return lax.div(block, 2) * 2 + (1 - lax.rem(block, 2))

    def add_product(block, first=False):
        part = dot(orb[block], ip[y, pl.ds(pl.multiple_of(block * COLS, COLS), COLS), :])
        product[...] = part if first else product[...] + part

    for load in loads[2:]:
        load.wait()
    gathered[...] = lax.dot_general(
        inv[...], occ[...], (((0,), (0,)), ((), ())), preferred_element_type=F32
    )
    add_product(place, True)
    pass_on(0)
    both("y0z")
    zs(0, -1)
    zs(0, 1)
    o_up[0].wait_recv()
    o_up2 = orb_copy(5, below, lower, on_y(1))
    o_up2.start()
    o_down[0].wait_recv()
    o_down2 = orb_copy(6, above, upper, on_y(-1))
    o_down2.start()
    y1z()
    y0x(1)
    pass_on(1)
    turn(y, 0, BASIS)
    o_up[1].wait_recv()
    o_across_below = orb_copy(7, below, everything, partner)
    o_across_below.start()
    o_down[1].wait_recv()
    o_across_above = orb_copy(8, above, everything, partner)
    o_across_above.start()
    pass_on(2)
    o_across.wait_recv()
    add_product(other(place))
    both("z0", -1)
    zs(1, -1)
    add_product(below)
    add_product(above)
    pass_on(3)
    o_across_below.wait_recv()
    add_product(other(below))
    o_across_above.wait_recv()
    add_product(other(above))
    o_up2.wait_recv()
    o_down2.wait_recv()
    o_across_far = orb_copy(9, far, everything, partner)
    o_across_far.start()
    both("z0", 1)
    zs(1, 1)
    add_product(far)
    y0x(-1)
    pass_on(4)
    o_across_far.wait_recv()
    add_product(other(far))

    weights[walk] = jnp.sum(gathered[...] * product[...], axis=0, keepdims=True)

    def send_weights(step, carry):
        pltpu.make_async_remote_copy(
            src_ref=weights.at[walk], dst_ref=weights.at[walk],
            send_sem=small_send.at[0], recv_sem=small_recv.at[0],
            device_id={"walk": lax.rem(walk + step, WALK), "chol": place}, device_id_type=MESH,
        ).start()
        return carry

    lax.fori_loop(1, WALK, send_weights, 0)
    both("y1z")
    zs(0, 2)
    both("y0x", 1)
    x0(-1, 1)
    x0(1, -1)
    both("z1", -1)
    zs(2, -1)
    both("z1", 1)
    zs(2, 1)
    both("y0x", -1)
    x0(-1, -1)
    x0(1, 1)
    y1x()
    y0c(1)
    window = pl.ds(pl.multiple_of(y * STEP, 16), WIN)
    for block in range(CHOL):
        rows = orb[block, window, :]
        term[:, block * COLS : (block + 1) * COLS] = rows
        total[:, block * COLS : (block + 1) * COLS] = rows.astype(F32)

    def multiply(block):
        current[block] = dot(term[...], ip[block])

    multiply(y)
    some = weights.at[pl.ds(0, WALK - 1)]
    pltpu.make_async_copy(some, some, small_recv.at[0]).wait()

    all_weights = weights[...].reshape(WALK, PTS)
    partial = sum_of_parts(dot(three_parts(all_weights), chol[...]), WALK)
    pair[core] = partial
    across = pltpu.make_async_remote_copy(
        src_ref=pair.at[core], dst_ref=pair.at[core],
        send_sem=small_send.at[4], recv_sem=small_recv.at[4],
        device_id=partner, device_id_type=MESH,
    )
    across.start()
    both("z0", 2)
    zs(1, 2)
    across.wait_recv()
    bias_parts[y] = pair[0] + pair[1]
    for step in (2, 1, 3):
        pltpu.make_async_remote_copy(
            src_ref=bias_parts.at[y], dst_ref=bias_parts.at[y],
            send_sem=small_send.at[1], recv_sem=small_recv.at[1],
            device_id=on_y(step), device_id_type=MESH,
        ).start()
    both("y1x")
    x0(2, 1)
    x0(2, -1)
    both("z2", -1)
    z3(-1)
    both("z2", 1)
    z3(1)
    y0c(-1)
    some_bias = bias_parts.at[pl.ds(0, NY - 1)]
    pltpu.make_async_copy(some_bias, some_bias, small_recv.at[1]).wait()
    bias[...] = (bias_parts[0] + bias_parts[1]) + (bias_parts[2] + bias_parts[3])

    coeff = TIME_ROOT * (fields[...] - bias[...])
    part = sum_of_parts(dot_last(three_parts(coeff), chol[...]), WALK)
    field_part[...] = part.reshape(WALK, 1, PTS)

    def send_scales(step, carry):
        to = lax.rem(walk + step, WALK)
        pltpu.make_async_remote_copy(
            src_ref=field_part.at[to], dst_ref=scale_in.at[walk],
            send_sem=small_send.at[2], recv_sem=small_recv.at[2],
            device_id={"walk": to, "chol": place}, device_id_type=MESH,
        ).start()
        return carry

    lax.fori_loop(1, WALK, send_scales, 0)
    scale_in[walk] = field_part[walk]
    both("z1", 2)
    zs(2, 2)
    for half in (1, -1):
        both("x0", -1, half)
        both("x0", 1, half)
    x1(-1)
    x1(1)
    both("y0c", 1)
    y1c()
    both("x0", 2, 1)
    both("x0", 2, -1)
    x1(2)
    both("z3", -1)
    both("z3", 1)
    for step in (-1, 1):
        turn(at_y(step), ZBASE, CBASE - ZBASE)
    both("z2", 2)
    z3(2)
    both("y0c", -1)
    for step in (-1, 1):
        turn(at_y(step), CBASE, CROWS)
    some_scales = scale_in.at[pl.ds(0, WALK - 1)]
    pltpu.make_async_copy(some_scales, some_scales, small_recv.at[2]).wait()
    scales[y] = jnp.sum(scale_in[...], axis=0)
    to_up = [
        pltpu.make_async_remote_copy(
            src_ref=scales.at[y], dst_ref=scales.at[y],
            send_sem=small_send.at[3], recv_sem=small_recv.at[3],
            device_id=on_y(step), device_id_type=MESH,
        )
        for step in range(1, NY)
    ]
    for copy in to_up:
        copy.start()

    both("x1", -1)
    both("x1", 1)
    for step in (-1, 1):
        turn(at_y(step), 0, ZBASE)
        multiply(at_y(step))
    both("y1c")
    both("z3", 2)
    turn(at_y(2), ZBASE, BASIS - ZBASE)
    both("x1", 2)
    turn(at_y(2), 0, ZBASE)
    multiply(at_y(2))
    some_blocks = scales.at[pl.ds(0, NY - 1)]
    pltpu.make_async_copy(some_blocks, some_blocks, small_recv.at[3]).wait()

    def exchange(slot, tile):
        return pltpu.make_async_remote_copy(
            src_ref=own_part.at[slot, tile], dst_ref=other_part.at[slot, tile],
            send_sem=part_send.at[slot, tile], recv_sem=part_recv.at[slot, tile],
            device_id=partner, device_id_type=MESH,
        )

    def mix(slot):
        for block in range(NY):
            mixed[:, block * PTS : (block + 1) * PTS] = (
                current[block] * (scales[block] / (slot + 1).astype(F32))
            ).astype(BF16)

    def points_to_basis(slot):
        mix(slot)
        for tile in range(TILES):
            columns = slice(tile * TILE, (tile + 1) * TILE)
            own_part[slot, tile] = dot(mixed[...], turned[:, columns]).astype(BF16)
            exchange(slot, tile).start()

    def summed(slot, tile):
        exchange(slot, tile).wait_recv()
        columns = slice(tile * TILE, (tile + 1) * TILE)
        value = (own_part[slot, tile].astype(F32) + other_part[slot, tile].astype(F32)).astype(BF16)
        total[:, columns] = total[:, columns] + value.astype(F32)
        return value

    def one_term(slot, carry):
        points_to_basis(slot)
        for tile in range(TILES):
            value = summed(slot, tile)
            for block in range(NY):
                part = dot(value, ip[block, tile * TILE : (tile + 1) * TILE, :])
                current[block] = current[block] + part if tile else part
        return carry

    lax.fori_loop(0, TERMS - 1, one_term, 0)
    last = TERMS - 1
    mix(jnp.int32(last))
    mine = pl.ds(pl.multiple_of(core * COLS, COLS), COLS)
    others = pl.ds(pl.multiple_of((1 - core) * COLS, COLS), COLS)

    def exchange_half(tile):
        return pltpu.make_async_remote_copy(
            src_ref=own_part.at[last, tile, :, others], dst_ref=other_part.at[last, tile, :, others],
            send_sem=part_send.at[last, tile], recv_sem=part_recv.at[last, tile],
            device_id=partner, device_id_type=MESH,
        )

    def begin(step):
        to = at_y(step)
        columns = pl.ds(pl.multiple_of(to * TILE, TILE), TILE)
        own_part[last, to] = dot(mixed[...], turned[:, columns]).astype(BF16)
        exchange_half(to).start()

    def finish(step):
        to = at_y(step)
        exchange_half(to).wait_recv()
        value = own_part[last, to, :, mine].astype(F32) + other_part[last, to, :, mine].astype(F32)
        columns = pl.ds(pl.multiple_of(to * TILE + core * COLS, COLS), COLS)
        row = (total[:, columns] + value.astype(BF16).astype(F32)).astype(BF16)
        if step:
            send_out[to] = row
            pltpu.make_async_remote_copy(
                src_ref=send_out.at[to], dst_ref=recv_out.at[y],
                send_sem=out_send, recv_sem=out_recv,
                device_id=on_y(step), device_id_type=MESH,
            ).start()
        else:
            recv_out[y] = row

    begin(2)
    begin(1)
    begin(3)
    finish(2)
    finish(1)
    begin(0)
    finish(3)
    finish(0)
    for copy in transfers.values():
        copy.wait_send()
    for copy in (*o_up, *o_down, o_across, o_up2, o_down2, o_across_below, o_across_above, o_across_far):
        copy.wait_send()
    pltpu.make_async_copy(some, some, small_send.at[0]).wait()
    pltpu.make_async_copy(some_bias, some_bias, small_send.at[1]).wait()
    pltpu.make_async_copy(some_scales, some_scales, small_send.at[2]).wait()
    pltpu.make_async_copy(some_blocks, some_blocks, small_send.at[3]).wait()
    across.wait_send()
    for slot in range(TERMS):
        for tile in range(TILES):
            (exchange if slot < last else lambda _, to: exchange_half(to))(slot, tile).wait_send()
    some_out = recv_out.at[pl.ds(0, NY - 1)]
    pltpu.make_async_copy(some_out, some_out, out_recv).wait()
    pltpu.make_async_copy(some_out, some_out, out_send).wait()


def assemble(parts, bias_in, out, bias_out):
    for part in range(NY):
        count = WIN if part == NY - 1 else STEP
        out[0, part * STEP : part * STEP + count] = parts[part, :count]
    bias_out[...] = bias_in[...]


N_GATHER = 16 + 18 + 24


def on_device(orbitals, intersection_inv, interp, occ_interp, chol_factors, fields):
    dma = pltpu.SemaphoreType.DMA
    hbm = pl.BlockSpec(memory_space=pltpu.HBM)
    vmem = pl.BlockSpec(memory_space=pltpu.VMEM)
    pieces = pl.pallas_call(
        kernel,
        out_shape=(
            jax.ShapeDtypeStruct((NY, WIN, COLS), BF16),
            jax.ShapeDtypeStruct((WALK, VEC), F32),
        ),
        in_specs=[hbm] * 6,
        out_specs=(vmem, vmem),
        scratch_shapes=[
            pltpu.VMEM((NY, BASIS, PTS), BF16),
            pltpu.VMEM((NY * PTS, BASIS), BF16),
            pltpu.VMEM((CHOL, ROWS, COLS), BF16),
            pltpu.VMEM((ROWS, ROWS), BF16),
            pltpu.VMEM((ROWS, PTS), BF16),
            pltpu.VMEM((PTS, VEC), BF16),
            pltpu.VMEM((WALK, VEC), F32),
            pltpu.VMEM((ROWS, PTS), F32),
            pltpu.VMEM((ROWS, PTS), F32),
            pltpu.VMEM((WALK, 1, PTS), F32),
            pltpu.VMEM((2, WALK, VEC), F32),
            pltpu.VMEM((NY, WALK, VEC), F32),
            pltpu.VMEM((WALK, 1, PTS), F32),
            pltpu.VMEM((WALK, 1, PTS), F32),
            pltpu.VMEM((NY, 1, PTS), F32),
            pltpu.VMEM((NY, WIN, PTS), F32),
            pltpu.VMEM((WIN, NY * PTS), BF16),
            pltpu.VMEM((TERMS, TILES, WIN, TILE), BF16),
            pltpu.VMEM((TERMS, TILES, WIN, TILE), BF16),
            pltpu.VMEM((WIN, BASIS), BF16),
            pltpu.VMEM((WIN, BASIS), F32),
            pltpu.VMEM((NY, WIN, COLS), BF16),
            dma((6,)),
            dma((N_GATHER,)),
            dma((N_GATHER,)),
            dma((10,)),
            dma((10,)),
            dma((5,)),
            dma((5,)),
            dma((TERMS, TILES)),
            dma((TERMS, TILES)),
            dma,
            dma,
            pltpu.SemaphoreType.REGULAR((NZ // 2 + 1,)),
        ],
        compiler_params=pltpu.CompilerParams(
            collective_id=0, has_side_effects=True, vmem_limit_bytes=44 * 1024 * 1024
        ),
    )(
        *(
            pltpu.with_memory_space_constraint(value, pltpu.HBM)
            for value in (orbitals, intersection_inv, interp, occ_interp, chol_factors, fields)
        )
    )
    return pl.pallas_call(
        assemble,
        out_shape=(
            jax.ShapeDtypeStruct((1, ROWS, COLS), BF16),
            jax.ShapeDtypeStruct((WALK, VEC), F32),
        ),
        in_specs=[vmem] * 2,
        out_specs=(vmem, vmem),
        compiler_params=pltpu.CompilerParams(vmem_limit_bytes=8 * 1024 * 1024),
    )(*pieces)


def solution(mesh):
    placed = (
        P("walk", None, "chol"),
        P("walk", None, None),
        P(None, "chol"),
        P(None, "chol"),
        P("chol", "walk"),
        P(None, "walk"),
    )
    return jax.shard_map(
        on_device,
        mesh=mesh,
        in_specs=placed,
        out_specs=(P("walk", None, "chol"), P(None, "walk")),
        check_vma=False,
    )
```

```python
import jax
import jax.numpy as jnp
from jax import lax
from jax.experimental import pallas as pl
from jax.experimental.pallas import tpu as pltpu
from jax.sharding import PartitionSpec as P

TERMS = 4
TIME_ROOT = 2.2
MESH = pl.DeviceIdType.MESH
F32, BF16 = jnp.float32, jnp.bfloat16

NX, NZ, NY = 4, 8, 4
WALK, CHOL = NX * NZ, NY * 2
ROWS, BASIS, PTS, VEC = 400, 2048, 512, 256
COLS = BASIS // CHOL
WIN, STEP = 112, 96
XROWS, XHALF = 192, 96
ZROWS, ZHALF = 96, 48
ZBASE = NX * XROWS
CBASE = ZBASE + NZ * ZROWS
CROWS, CHALF = BASIS - CBASE, 256
TILE = 512
TILES = BASIS // TILE
TURN = 512


def three_parts(value):
    high = value.astype(BF16)
    rest = value - high.astype(F32)
    middle = rest.astype(BF16)
    low = (rest - middle.astype(F32)).astype(BF16)
    return jnp.concatenate([high, middle, low], axis=0)


def sum_of_parts(value, rows):
    return value[:rows] + value[rows : 2 * rows] + value[2 * rows :]


def dot(left, right):
    return jnp.dot(left, right, preferred_element_type=F32)


def dot_last(left, right):
    return lax.dot_general(left, right, (((1,), (1,)), ((), ())), preferred_element_type=F32)


def kernel(
    orb_in, inv_in, interp_in, occ_in, chol_in, fields_in,
    recv_out, bias,
    ip, turned, orb, inv, occ, chol, fields,
    gathered, product, weights, pair, bias_parts, field_part, scale_in, scales,
    current, mixed, own_part, other_part, term, total, send_out,
    load_sem, gather_send, gather_recv, orb_send, orb_recv,
    small_send, small_recv, part_send, part_recv, out_send, out_recv, ready,
):
    walk, place = lax.axis_index("walk"), lax.axis_index("chol")
    x, z = lax.rem(walk, NX), lax.div(walk, NX)
    core, y = lax.rem(place, 2), lax.div(place, 2)

    def at_y(step):
        return lax.rem(y + step + NY, NY)

    def chol_of(step):
        return at_y(step) * 2 + core

    def on_x(step):
        return {"walk": z * NX + lax.rem(x + step + NX, NX), "chol": place}

    def on_z(step):
        return {"walk": lax.rem(z + step + NZ, NZ) * NX + x, "chol": place}

    def on_y(step):
        return {"walk": walk, "chol": chol_of(step)}

    partner = {"walk": walk, "chol": y * 2 + (1 - core)}

    barrier = pltpu.get_barrier_semaphore()

    loads = [
        pltpu.make_async_copy(orb_in.at[0], orb.at[place], load_sem.at[0]),
        pltpu.make_async_copy(interp_in, ip.at[y], load_sem.at[1]),
        pltpu.make_async_copy(inv_in.at[0], inv, load_sem.at[2]),
        pltpu.make_async_copy(occ_in, occ, load_sem.at[3]),
        pltpu.make_async_copy(chol_in, chol, load_sem.at[4]),
        pltpu.make_async_copy(fields_in, fields, load_sem.at[5]),
    ]
    for load in loads:
        load.start()
    neighbours = [on_x(1), on_x(-1), on_z(1), on_z(-1)]

    def greet(step, carry):
        pl.semaphore_signal(
            barrier, inc=1,
            device_id={"walk": walk, "chol": lax.rem(place + step, CHOL)}, device_id_type=MESH,
        )
        return carry

    for device in neighbours:
        pl.semaphore_signal(barrier, inc=1, device_id=device, device_id_type=MESH)
    lax.fori_loop(1, CHOL, greet, 0)

    def tell(index, devices):
        for device in devices:
            pl.semaphore_signal(ready.at[index], inc=1, device_id=device, device_id_type=MESH)

    def pass_on(index):
        pl.semaphore_wait(ready.at[index], 2)
        if index < NZ // 2:
            tell(index + 1, neighbours[2:])
    def turn(block, first, count):
        points = pl.ds(pl.multiple_of(block * PTS, PTS), PTS)
        for start in range(first, first + count, TURN):
            rows = slice(start, min(start + TURN, first + count))
            turned[points, rows] = ip[block, rows, :].T

    pl.semaphore_wait(barrier, CHOL - 1 + len(neighbours))
    loads[0].wait()
    loads[1].wait()

    def moved(index, block, start, count, device):
        place_of = ip.at[block, pl.ds(pl.multiple_of(start, 16), count)]
        return pltpu.make_async_remote_copy(
            src_ref=place_of, dst_ref=place_of,
            send_sem=gather_send.at[index], recv_sem=gather_recv.at[index],
            device_id=device, device_id_type=MESH,
        )

    transfers = {}

    def start_gather(name, *what):
        copy = moved(len(transfers), *what)
        transfers[name] = copy
        copy.start()

    def landed(*names):
        for name in names:
            transfers[name].wait_recv()

    def x_piece(step):
        return lax.rem(x + step + NX, NX) * XROWS

    def z_piece(step):
        return ZBASE + lax.rem(z + step + NZ, NZ) * ZROWS

    def half_of(start, rows, half, way):
        return (start, half) if way == 1 else (start + half, rows - half)

    def x_half(step, way):
        return half_of(x_piece(step), XROWS, XHALF, way)

    def z_half(step, way):
        return half_of(z_piece(step), ZROWS, ZHALF, way)

    def c_half(way):
        return half_of(CBASE, CROWS, CHALF, way)

    def y0z():
        for way in (1, -1):
            start_gather(("y0z", way), y, z_piece(0), ZROWS, on_y(way))

    def y0x(first):
        for way in (1, -1):
            start_gather(("y0x", first, way), y, *x_half(0, way * first), on_y(way))

    def y0c(first):
        for way in (1, -1):
            start_gather(("y0c", first, way), y, *c_half(way * first), on_y(way))

    def y1z():
        for way in (1, -1):
            start_gather(("y1z", way), at_y(-way), *z_half(0, way), on_y(way))

    def y1x():
        for way in (1, -1):
            start_gather(("y1x", way), at_y(-way), *x_half(0, way), on_y(way))

    def y1c():
        for way in (1, -1):
            start_gather(("y1c", way), at_y(-way), *c_half(way), on_y(way))

    def x0(block, half):
        for way in (half, -half):
            start_gather(("x0", block, half, way), at_y(block), *x_half(0, half), on_x(way))

    def x1(block):
        for way in (1, -1):
            start_gather(("x1", block, way), at_y(block), *x_half(-way, way), on_x(way))

    def zs(step, block):
        for way in (1, -1):
            start_gather(
                (f"z{step}", block, way), at_y(block), z_piece(-way * step), ZROWS, on_z(way)
            )

    def z3(block):
        for way in (1, -1):
            start_gather(("z3", block, way), at_y(block), *z_half(-3 * way, way), on_z(way))

    def both(*stage):
        landed((*stage, 1), (*stage, -1))

    def orb_copy(index, block, rows, device):
        place_of = orb.at[block, rows]
        return pltpu.make_async_remote_copy(
            src_ref=place_of, dst_ref=place_of,
            send_sem=orb_send.at[index], recv_sem=orb_recv.at[index],
            device_id=device, device_id_type=MESH,
        )

    everything, lower, upper = pl.ds(0, ROWS), pl.ds(0, 208), pl.ds(208, 192)
    below, above, far = chol_of(-1), chol_of(1), chol_of(2)
    o_up = [orb_copy(0, place, lower, on_y(1)), orb_copy(1, place, upper, on_y(1))]
    o_down = [orb_copy(2, place, upper, on_y(-1)), orb_copy(3, place, lower, on_y(-1))]
    o_across = orb_copy(4, place, everything, partner)
    y0z()
    for copy in (o_up[0], o_down[0], o_up[1], o_down[1], o_across):
        copy.start()
    tell(0, neighbours[:2])

    def other(block):
        return lax.div(block, 2) * 2 + (1 - lax.rem(block, 2))

    def add_product(block, first=False):
        part = dot(orb[block], ip[y, pl.ds(pl.multiple_of(block * COLS, COLS), COLS), :])
        product[...] = part if first else product[...] + part

    for load in loads[2:]:
        load.wait()
    gathered[...] = lax.dot_general(
        inv[...], occ[...], (((0,), (0,)), ((), ())), preferred_element_type=F32
    )
    add_product(place, True)
    pass_on(0)
    both("y0z")
    zs(0, -1)
    zs(0, 1)
    o_up[0].wait_recv()
    o_up2 = orb_copy(5, below, lower, on_y(1))
    o_up2.start()
    o_down[0].wait_recv()
    o_down2 = orb_copy(6, above, upper, on_y(-1))
    o_down2.start()
    y1z()
    y0x(1)
    pass_on(1)
    turn(y, 0, BASIS)
    o_up[1].wait_recv()
    o_across_below = orb_copy(7, below, everything, partner)
    o_across_below.start()
    o_down[1].wait_recv()
    o_across_above = orb_copy(8, above, everything, partner)
    o_across_above.start()
    pass_on(2)
    o_across.wait_recv()
    add_product(other(place))
    both("z0", -1)
    zs(1, -1)
    add_product(below)
    add_product(above)
    pass_on(3)
    o_across_below.wait_recv()
    add_product(other(below))
    o_across_above.wait_recv()
    add_product(other(above))
    o_up2.wait_recv()
    o_down2.wait_recv()
    o_across_far = orb_copy(9, far, everything, partner)
    o_across_far.start()
    both("z0", 1)
    zs(1, 1)
    add_product(far)
    y0x(-1)
    pass_on(4)
    o_across_far.wait_recv()
    add_product(other(far))

    def far_first(index):
        away = lax.div(index + 1, 2) * (1 - 2 * lax.rem(index, 2))
        return lax.rem(walk + WALK // 2 + away, WALK)

    weights[walk] = jnp.sum(gathered[...] * product[...], axis=0, keepdims=True)

    def send_weights(index, carry):
        pltpu.make_async_remote_copy(
            src_ref=weights.at[walk], dst_ref=weights.at[walk],
            send_sem=small_send.at[0], recv_sem=small_recv.at[0],
            device_id={"walk": far_first(index), "chol": place}, device_id_type=MESH,
        ).start()
        return carry

    lax.fori_loop(0, WALK - 1, send_weights, 0)
    both("y1z")
    zs(0, 2)
    both("y0x", 1)
    x0(-1, 1)
    x0(1, -1)
    both("z1", -1)
    zs(2, -1)
    both("z1", 1)
    zs(2, 1)
    both("y0x", -1)
    x0(-1, -1)
    x0(1, 1)
    y1x()
    y0c(1)
    window = pl.ds(pl.multiple_of(y * STEP, 16), WIN)
    for block in range(CHOL):
        rows = orb[block, window, :]
        term[:, block * COLS : (block + 1) * COLS] = rows
        total[:, block * COLS : (block + 1) * COLS] = rows.astype(F32)

    def multiply(block, start, count, first=False):
        rows = slice(start, start + count)
        part = dot(term[:, rows], ip[block, rows, :])
        current[block] = part if first else current[block] + part

    x_rows, z_rows, c_rows = (0, ZBASE), (ZBASE, CBASE - ZBASE), (CBASE, CROWS)

    def use(step, rows, first=False):
        turn(at_y(step), *rows)
        multiply(at_y(step), *rows, first)

    multiply(y, 0, BASIS, True)
    some = weights.at[pl.ds(0, WALK - 1)]
    pltpu.make_async_copy(some, some, small_recv.at[0]).wait()

    all_weights = weights[...].reshape(WALK, PTS)
    partial = sum_of_parts(dot(three_parts(all_weights), chol[...]), WALK)
    pair[core] = partial
    across = pltpu.make_async_remote_copy(
        src_ref=pair.at[core], dst_ref=pair.at[core],
        send_sem=small_send.at[4], recv_sem=small_recv.at[4],
        device_id=partner, device_id_type=MESH,
    )
    across.start()
    both("z0", 2)
    zs(1, 2)
    across.wait_recv()
    bias_parts[y] = pair[0] + pair[1]
    for step in (2, 1, 3):
        pltpu.make_async_remote_copy(
            src_ref=bias_parts.at[y], dst_ref=bias_parts.at[y],
            send_sem=small_send.at[1], recv_sem=small_recv.at[1],
            device_id=on_y(step), device_id_type=MESH,
        ).start()
    both("y1x")
    x0(2, 1)
    x0(2, -1)
    both("z2", -1)
    z3(-1)
    both("z2", 1)
    z3(1)
    y0c(-1)
    some_bias = bias_parts.at[pl.ds(0, NY - 1)]
    pltpu.make_async_copy(some_bias, some_bias, small_recv.at[1]).wait()
    bias[...] = (bias_parts[0] + bias_parts[1]) + (bias_parts[2] + bias_parts[3])

    coeff = TIME_ROOT * (fields[...] - bias[...])
    part = sum_of_parts(dot_last(three_parts(coeff), chol[...]), WALK)
    field_part[...] = part.reshape(WALK, 1, PTS)

    def send_scales(index, carry):
        to = far_first(index)
        pltpu.make_async_remote_copy(
            src_ref=field_part.at[to], dst_ref=scale_in.at[walk],
            send_sem=small_send.at[2], recv_sem=small_recv.at[2],
            device_id={"walk": to, "chol": place}, device_id_type=MESH,
        ).start()
        return carry

    lax.fori_loop(0, WALK - 1, send_scales, 0)
    scale_in[walk] = field_part[walk]
    both("z1", 2)
    zs(2, 2)
    for half in (1, -1):
        both("x0", -1, half)
        both("x0", 1, half)
    x1(-1)
    x1(1)
    both("y0c", 1)
    y1c()
    both("x0", 2, 1)
    both("x0", 2, -1)
    x1(2)
    both("z3", -1)
    both("z3", 1)
    use(-1, z_rows, True)
    use(1, z_rows, True)
    both("z2", 2)
    z3(2)
    both("y0c", -1)
    use(-1, c_rows)
    use(1, c_rows)
    some_scales = scale_in.at[pl.ds(0, WALK - 1)]
    pltpu.make_async_copy(some_scales, some_scales, small_recv.at[2]).wait()
    scales[y] = jnp.sum(scale_in[...], axis=0)
    to_up = [
        pltpu.make_async_remote_copy(
            src_ref=scales.at[y], dst_ref=scales.at[y],
            send_sem=small_send.at[3], recv_sem=small_recv.at[3],
            device_id=on_y(step), device_id_type=MESH,
        )
        for step in range(1, NY)
    ]
    for copy in to_up:
        copy.start()

    both("x1", -1)
    both("x1", 1)
    use(-1, x_rows)
    use(1, x_rows)
    both("y1c")
    use(2, c_rows, True)
    both("x1", 2)
    use(2, x_rows)
    both("z3", 2)
    use(2, z_rows)
    some_blocks = scales.at[pl.ds(0, NY - 1)]
    pltpu.make_async_copy(some_blocks, some_blocks, small_recv.at[3]).wait()

    def exchange(slot, tile):
        return pltpu.make_async_remote_copy(
            src_ref=own_part.at[slot, tile], dst_ref=other_part.at[slot, tile],
            send_sem=part_send.at[slot, tile], recv_sem=part_recv.at[slot, tile],
            device_id=partner, device_id_type=MESH,
        )

    def mix(slot):
        for block in range(NY):
            mixed[:, block * PTS : (block + 1) * PTS] = (
                current[block] * (scales[block] / (slot + 1).astype(F32))
            ).astype(BF16)

    def points_to_basis(slot):
        mix(slot)
        for pair_of in range(0, TILES, 2):
            columns = slice(pair_of * TILE, (pair_of + 2) * TILE)
            value = dot(mixed[:, :PTS], turned[:PTS, columns])
            for block in range(1, NY):
                points = slice(block * PTS, (block + 1) * PTS)
                value += dot(mixed[:, points], turned[points, columns])
            for tile in (pair_of, pair_of + 1):
                first = (tile - pair_of) * TILE
                own_part[slot, tile] = value[:, first : first + TILE].astype(BF16)
                exchange(slot, tile).start()

    def summed(slot, tile):
        exchange(slot, tile).wait_recv()
        columns = slice(tile * TILE, (tile + 1) * TILE)
        value = (own_part[slot, tile].astype(F32) + other_part[slot, tile].astype(F32)).astype(BF16)
        total[:, columns] = total[:, columns] + value.astype(F32)
        return value

    def one_term(slot, carry):
        points_to_basis(slot)
        for tile in range(TILES):
            value = summed(slot, tile)
            for block in range(NY):
                part = dot(value, ip[block, tile * TILE : (tile + 1) * TILE, :])
                current[block] = current[block] + part if tile else part
        return carry

    lax.fori_loop(0, TERMS - 1, one_term, 0)
    last = TERMS - 1
    mix(jnp.int32(last))
    mine = pl.ds(pl.multiple_of(core * COLS, COLS), COLS)
    others = pl.ds(pl.multiple_of((1 - core) * COLS, COLS), COLS)

    def exchange_half(tile):
        return pltpu.make_async_remote_copy(
            src_ref=own_part.at[last, tile, :, others], dst_ref=other_part.at[last, tile, :, others],
            send_sem=part_send.at[last, tile], recv_sem=part_recv.at[last, tile],
            device_id=partner, device_id_type=MESH,
        )

    def begin(step):
        to = at_y(step)
        columns = pl.ds(pl.multiple_of(to * TILE, TILE), TILE)
        own_part[last, to] = dot(mixed[...], turned[:, columns]).astype(BF16)
        exchange_half(to).start()

    def finish(step):
        to = at_y(step)
        exchange_half(to).wait_recv()
        value = own_part[last, to, :, mine].astype(F32) + other_part[last, to, :, mine].astype(F32)
        columns = pl.ds(pl.multiple_of(to * TILE + core * COLS, COLS), COLS)
        row = (total[:, columns] + value.astype(BF16).astype(F32)).astype(BF16)
        if step:
            send_out[to] = row
            pltpu.make_async_remote_copy(
                src_ref=send_out.at[to], dst_ref=recv_out.at[y],
                send_sem=out_send, recv_sem=out_recv,
                device_id=on_y(step), device_id_type=MESH,
            ).start()
        else:
            recv_out[y] = row

    begin(2)
    begin(1)
    begin(3)
    finish(2)
    finish(1)
    begin(0)
    finish(3)
    finish(0)
    for copy in transfers.values():
        copy.wait_send()
    for copy in (*o_up, *o_down, o_across, o_up2, o_down2, o_across_below, o_across_above, o_across_far):
        copy.wait_send()
    pltpu.make_async_copy(some, some, small_send.at[0]).wait()
    pltpu.make_async_copy(some_bias, some_bias, small_send.at[1]).wait()
    pltpu.make_async_copy(some_scales, some_scales, small_send.at[2]).wait()
    pltpu.make_async_copy(some_blocks, some_blocks, small_send.at[3]).wait()
    across.wait_send()
    for slot in range(TERMS):
        for tile in range(TILES):
            (exchange if slot < last else lambda _, to: exchange_half(to))(slot, tile).wait_send()
    some_out = recv_out.at[pl.ds(0, NY - 1)]
    pltpu.make_async_copy(some_out, some_out, out_recv).wait()
    pltpu.make_async_copy(some_out, some_out, out_send).wait()


def assemble(parts, bias_in, out, bias_out):
    for part in range(NY):
        count = WIN if part == NY - 1 else STEP
        out[0, part * STEP : part * STEP + count] = parts[part, :count]
    bias_out[...] = bias_in[...]


N_GATHER = 16 + 18 + 24


def on_device(orbitals, intersection_inv, interp, occ_interp, chol_factors, fields):
    dma = pltpu.SemaphoreType.DMA
    hbm = pl.BlockSpec(memory_space=pltpu.HBM)
    vmem = pl.BlockSpec(memory_space=pltpu.VMEM)
    pieces = pl.pallas_call(
        kernel,
        out_shape=(
            jax.ShapeDtypeStruct((NY, WIN, COLS), BF16),
            jax.ShapeDtypeStruct((WALK, VEC), F32),
        ),
        in_specs=[hbm] * 6,
        out_specs=(vmem, vmem),
        scratch_shapes=[
            pltpu.VMEM((NY, BASIS, PTS), BF16),
            pltpu.VMEM((NY * PTS, BASIS), BF16),
            pltpu.VMEM((CHOL, ROWS, COLS), BF16),
            pltpu.VMEM((ROWS, ROWS), BF16),
            pltpu.VMEM((ROWS, PTS), BF16),
            pltpu.VMEM((PTS, VEC), BF16),
            pltpu.VMEM((WALK, VEC), F32),
            pltpu.VMEM((ROWS, PTS), F32),
            pltpu.VMEM((ROWS, PTS), F32),
            pltpu.VMEM((WALK, 1, PTS), F32),
            pltpu.VMEM((2, WALK, VEC), F32),
            pltpu.VMEM((NY, WALK, VEC), F32),
            pltpu.VMEM((WALK, 1, PTS), F32),
            pltpu.VMEM((WALK, 1, PTS), F32),
            pltpu.VMEM((NY, 1, PTS), F32),
            pltpu.VMEM((NY, WIN, PTS), F32),
            pltpu.VMEM((WIN, NY * PTS), BF16),
            pltpu.VMEM((TERMS, TILES, WIN, TILE), BF16),
            pltpu.VMEM((TERMS, TILES, WIN, TILE), BF16),
            pltpu.VMEM((WIN, BASIS), BF16),
            pltpu.VMEM((WIN, BASIS), F32),
            pltpu.VMEM((NY, WIN, COLS), BF16),
            dma((6,)),
            dma((N_GATHER,)),
            dma((N_GATHER,)),
            dma((10,)),
            dma((10,)),
            dma((5,)),
            dma((5,)),
            dma((TERMS, TILES)),
            dma((TERMS, TILES)),
            dma,
            dma,
            pltpu.SemaphoreType.REGULAR((NZ // 2 + 1,)),
        ],
        compiler_params=pltpu.CompilerParams(
            collective_id=0, has_side_effects=True, vmem_limit_bytes=44 * 1024 * 1024
        ),
    )(
        *(
            pltpu.with_memory_space_constraint(value, pltpu.HBM)
            for value in (orbitals, intersection_inv, interp, occ_interp, chol_factors, fields)
        )
    )
    return pl.pallas_call(
        assemble,
        out_shape=(
            jax.ShapeDtypeStruct((1, ROWS, COLS), BF16),
            jax.ShapeDtypeStruct((WALK, VEC), F32),
        ),
        in_specs=[vmem] * 2,
        out_specs=(vmem, vmem),
        compiler_params=pltpu.CompilerParams(vmem_limit_bytes=8 * 1024 * 1024),
    )(*pieces)


def solution(mesh):
    placed = (
        P("walk", None, "chol"),
        P("walk", None, None),
        P(None, "chol"),
        P(None, "chol"),
        P("chol", "walk"),
        P(None, "walk"),
    )
    return jax.shard_map(
        on_device,
        mesh=mesh,
        in_specs=placed,
        out_specs=(P("walk", None, "chol"), P(None, "walk")),
        check_vma=False,
    )
```

```python
import jax
import jax.numpy as jnp
from jax import lax
from jax.experimental import pallas as pl
from jax.experimental.pallas import tpu as pltpu
from jax.sharding import PartitionSpec as P

TERMS = 4
TIME_ROOT = 2.2
MESH = pl.DeviceIdType.MESH
F32, BF16 = jnp.float32, jnp.bfloat16

NX, NZ, NY = 4, 8, 4
WALK, CHOL = NX * NZ, NY * 2
ROWS, BASIS, PTS, VEC = 400, 2048, 512, 256
COLS = BASIS // CHOL
WIN, STEP = 112, 96
XROWS, XHALF = 192, 96
ZROWS, ZHALF = 96, 48
ZBASE = NX * XROWS
CBASE = ZBASE + NZ * ZROWS
CROWS, CHALF = BASIS - CBASE, 256
TILE = 512
TILES = BASIS // TILE
TURN = 512


def three_parts(value):
    high = value.astype(BF16)
    rest = value - high.astype(F32)
    middle = rest.astype(BF16)
    low = (rest - middle.astype(F32)).astype(BF16)
    return jnp.concatenate([high, middle, low], axis=0)


def sum_of_parts(value, rows):
    return value[:rows] + value[rows : 2 * rows] + value[2 * rows :]


def dot(left, right):
    return jnp.dot(left, right, preferred_element_type=F32)


def dot_last(left, right):
    return lax.dot_general(left, right, (((1,), (1,)), ((), ())), preferred_element_type=F32)


def kernel(
    orb_in, inv_in, interp_in, occ_in, chol_in, fields_in,
    recv_out, bias,
    ip, turned, orb, inv, occ, chol, fields,
    gathered, product, weights, pair, bias_parts, field_part, scale_in, scales,
    current, mixed, own_part, other_part, term, total, send_out,
    load_sem, gather_send, gather_recv, orb_send, orb_recv,
    small_send, small_recv, part_send, part_recv, out_send, out_recv, ready,
):
    walk, place = lax.axis_index("walk"), lax.axis_index("chol")
    x, z = lax.rem(walk, NX), lax.div(walk, NX)
    core, y = lax.rem(place, 2), lax.div(place, 2)

    def at_y(step):
        return lax.rem(y + step + NY, NY)

    def chol_of(step):
        return at_y(step) * 2 + core

    def on_x(step):
        return {"walk": z * NX + lax.rem(x + step + NX, NX), "chol": place}

    def on_z(step):
        return {"walk": lax.rem(z + step + NZ, NZ) * NX + x, "chol": place}

    def on_y(step):
        return {"walk": walk, "chol": chol_of(step)}

    partner = {"walk": walk, "chol": y * 2 + (1 - core)}

    barrier = pltpu.get_barrier_semaphore()

    loads = [
        pltpu.make_async_copy(orb_in.at[0], orb.at[place], load_sem.at[0]),
        pltpu.make_async_copy(interp_in, ip.at[y], load_sem.at[1]),
        pltpu.make_async_copy(inv_in.at[0], inv, load_sem.at[2]),
        pltpu.make_async_copy(occ_in, occ, load_sem.at[3]),
        pltpu.make_async_copy(chol_in, chol, load_sem.at[4]),
        pltpu.make_async_copy(fields_in, fields, load_sem.at[5]),
    ]
    for load in loads:
        load.start()
    neighbours = [on_x(1), on_x(-1), on_z(1), on_z(-1)]

    def greet(step, carry):
        pl.semaphore_signal(
            barrier, inc=1,
            device_id={"walk": walk, "chol": lax.rem(place + step, CHOL)}, device_id_type=MESH,
        )
        return carry

    for device in neighbours:
        pl.semaphore_signal(barrier, inc=1, device_id=device, device_id_type=MESH)
    lax.fori_loop(1, CHOL, greet, 0)

    def tell(index, devices):
        for device in devices:
            pl.semaphore_signal(ready.at[index], inc=1, device_id=device, device_id_type=MESH)

    def pass_on(index):
        pl.semaphore_wait(ready.at[index], 2)
        if index < NZ // 2:
            tell(index + 1, neighbours[2:])
    def turn(block, first, count):
        points = pl.ds(pl.multiple_of(block * PTS, PTS), PTS)
        for start in range(first, first + count, TURN):
            rows = slice(start, min(start + TURN, first + count))
            turned[points, rows] = ip[block, rows, :].T

    pl.semaphore_wait(barrier, CHOL - 1 + len(neighbours))
    loads[0].wait()
    loads[1].wait()

    def moved(index, block, start, count, device):
        place_of = ip.at[block, pl.ds(pl.multiple_of(start, 16), count)]
        return pltpu.make_async_remote_copy(
            src_ref=place_of, dst_ref=place_of,
            send_sem=gather_send.at[index], recv_sem=gather_recv.at[index],
            device_id=device, device_id_type=MESH,
        )

    transfers = {}

    def start_gather(name, *what):
        copy = moved(len(transfers), *what)
        transfers[name] = copy
        copy.start()

    def landed(*names):
        for name in names:
            transfers[name].wait_recv()

    def x_piece(step):
        return lax.rem(x + step + NX, NX) * XROWS

    def z_piece(step):
        return ZBASE + lax.rem(z + step + NZ, NZ) * ZROWS

    def half_of(start, rows, half, way):
        return (start, half) if way == 1 else (start + half, rows - half)

    def x_half(step, way):
        return half_of(x_piece(step), XROWS, XHALF, way)

    def z_half(step, way):
        return half_of(z_piece(step), ZROWS, ZHALF, way)

    def c_half(way):
        return half_of(CBASE, CROWS, CHALF, way)

    def y0z():
        for way in (1, -1):
            start_gather(("y0z", way), y, z_piece(0), ZROWS, on_y(way))

    def y0x(first):
        for way in (1, -1):
            start_gather(("y0x", first, way), y, *x_half(0, way * first), on_y(way))

    def y0c(first):
        for way in (1, -1):
            start_gather(("y0c", first, way), y, *c_half(way * first), on_y(way))

    def y1z():
        for way in (1, -1):
            start_gather(("y1z", way), at_y(-way), *z_half(0, way), on_y(way))

    def y1x():
        for way in (1, -1):
            start_gather(("y1x", way), at_y(-way), *x_half(0, way), on_y(way))

    def y1c():
        for way in (1, -1):
            start_gather(("y1c", way), at_y(-way), *c_half(way), on_y(way))

    def x0(block, half):
        for way in (half, -half):
            start_gather(("x0", block, half, way), at_y(block), *x_half(0, half), on_x(way))

    def x1(block):
        for way in (1, -1):
            start_gather(("x1", block, way), at_y(block), *x_half(-way, way), on_x(way))

    def zs(step, block):
        for way in (1, -1):
            start_gather(
                (f"z{step}", block, way), at_y(block), z_piece(-way * step), ZROWS, on_z(way)
            )

    def z3(block):
        for way in (1, -1):
            start_gather(("z3", block, way), at_y(block), *z_half(-3 * way, way), on_z(way))

    def both(*stage):
        landed((*stage, 1), (*stage, -1))

    def orb_copy(index, block, rows, device):
        place_of = orb.at[block, rows]
        return pltpu.make_async_remote_copy(
            src_ref=place_of, dst_ref=place_of,
            send_sem=orb_send.at[index], recv_sem=orb_recv.at[index],
            device_id=device, device_id_type=MESH,
        )

    everything, lower, upper = pl.ds(0, ROWS), pl.ds(0, 208), pl.ds(208, 192)
    below, above, far = chol_of(-1), chol_of(1), chol_of(2)
    o_up = [orb_copy(0, place, lower, on_y(1)), orb_copy(1, place, upper, on_y(1))]
    o_down = [orb_copy(2, place, upper, on_y(-1)), orb_copy(3, place, lower, on_y(-1))]
    o_across = orb_copy(4, place, everything, partner)
    y0z()
    for copy in (o_up[0], o_down[0], o_up[1], o_down[1], o_across):
        copy.start()
    tell(0, neighbours[:2])

    def other(block):
        return lax.div(block, 2) * 2 + (1 - lax.rem(block, 2))

    def add_product(block, first=False):
        part = dot(orb[block], ip[y, pl.ds(pl.multiple_of(block * COLS, COLS), COLS), :])
        product[...] = part if first else product[...] + part

    for load in loads[2:]:
        load.wait()
    gathered[...] = lax.dot_general(
        inv[...], occ[...], (((0,), (0,)), ((), ())), preferred_element_type=F32
    )
    add_product(place, True)
    pass_on(0)
    both("y0z")
    zs(0, -1)
    zs(0, 1)
    o_up[0].wait_recv()
    o_up2 = orb_copy(5, below, lower, on_y(1))
    o_up2.start()
    o_down[0].wait_recv()
    o_down2 = orb_copy(6, above, upper, on_y(-1))
    o_down2.start()
    y1z()
    y0x(1)
    pass_on(1)
    turn(y, 0, BASIS)
    o_up[1].wait_recv()
    o_across_below = orb_copy(7, below, everything, partner)
    o_across_below.start()
    o_down[1].wait_recv()
    o_across_above = orb_copy(8, above, everything, partner)
    o_across_above.start()
    pass_on(2)
    o_across.wait_recv()
    add_product(other(place))
    both("z0", -1)
    zs(1, -1)
    add_product(below)
    add_product(above)
    pass_on(3)
    o_across_below.wait_recv()
    add_product(other(below))
    o_across_above.wait_recv()
    add_product(other(above))
    o_up2.wait_recv()
    o_down2.wait_recv()
    o_across_far = orb_copy(9, far, everything, partner)
    o_across_far.start()
    both("z0", 1)
    zs(1, 1)
    add_product(far)
    y0x(-1)
    pass_on(4)
    o_across_far.wait_recv()
    add_product(other(far))

    def far_first(index):
        away = lax.div(index + 1, 2) * (1 - 2 * lax.rem(index, 2))
        return lax.rem(walk + WALK // 2 + away, WALK)

    weights[walk] = jnp.sum(gathered[...] * product[...], axis=0, keepdims=True)

    def send_weights(index, carry):
        pltpu.make_async_remote_copy(
            src_ref=weights.at[walk], dst_ref=weights.at[walk],
            send_sem=small_send.at[0], recv_sem=small_recv.at[0],
            device_id={"walk": far_first(index), "chol": place}, device_id_type=MESH,
        ).start()
        return carry

    lax.fori_loop(0, WALK - 1, send_weights, 0)
    both("y1z")
    zs(0, 2)
    both("y0x", 1)
    x0(-1, 1)
    x0(1, -1)
    both("z1", -1)
    zs(2, -1)
    both("z1", 1)
    zs(2, 1)
    both("y0x", -1)
    x0(-1, -1)
    x0(1, 1)
    y1x()
    y0c(1)
    window = pl.ds(pl.multiple_of(y * STEP, 16), WIN)
    for block in range(CHOL):
        rows = orb[block, window, :]
        term[:, block * COLS : (block + 1) * COLS] = rows
        total[:, block * COLS : (block + 1) * COLS] = rows.astype(F32)

    def multiply(block, start, count, first=False):
        rows = slice(start, start + count)
        part = dot(term[:, rows], ip[block, rows, :])
        current[block] = part if first else current[block] + part

    x_rows, z_rows, c_rows = (0, ZBASE), (ZBASE, CBASE - ZBASE), (CBASE, CROWS)

    def use(step, rows, first=False):
        turn(at_y(step), *rows)
        multiply(at_y(step), *rows, first)

    multiply(y, 0, BASIS, True)
    some = weights.at[pl.ds(0, WALK - 1)]
    pltpu.make_async_copy(some, some, small_recv.at[0]).wait()

    all_weights = weights[...].reshape(WALK, PTS)
    partial = sum_of_parts(dot(three_parts(all_weights), chol[...]), WALK)
    pair[core] = partial
    across = pltpu.make_async_remote_copy(
        src_ref=pair.at[core], dst_ref=pair.at[core],
        send_sem=small_send.at[4], recv_sem=small_recv.at[4],
        device_id=partner, device_id_type=MESH,
    )
    across.start()
    both("z0", 2)
    zs(1, 2)
    across.wait_recv()
    bias_parts[y] = pair[0] + pair[1]
    for step in (2, 1, 3):
        pltpu.make_async_remote_copy(
            src_ref=bias_parts.at[y], dst_ref=bias_parts.at[y],
            send_sem=small_send.at[1], recv_sem=small_recv.at[1],
            device_id=on_y(step), device_id_type=MESH,
        ).start()
    both("y1x")
    x0(2, 1)
    x0(2, -1)
    both("z2", -1)
    z3(-1)
    both("z2", 1)
    z3(1)
    y0c(-1)
    some_bias = bias_parts.at[pl.ds(0, NY - 1)]
    pltpu.make_async_copy(some_bias, some_bias, small_recv.at[1]).wait()
    bias[...] = (bias_parts[0] + bias_parts[1]) + (bias_parts[2] + bias_parts[3])

    coeff = TIME_ROOT * (fields[...] - bias[...])
    part = sum_of_parts(dot_last(three_parts(coeff), chol[...]), WALK)
    field_part[...] = part.reshape(WALK, 1, PTS)

    def send_scales(index, carry):
        to = far_first(index)
        pltpu.make_async_remote_copy(
            src_ref=field_part.at[to], dst_ref=scale_in.at[walk],
            send_sem=small_send.at[2], recv_sem=small_recv.at[2],
            device_id={"walk": to, "chol": place}, device_id_type=MESH,
        ).start()
        return carry

    lax.fori_loop(0, WALK - 1, send_scales, 0)
    scale_in[walk] = field_part[walk]
    both("z1", 2)
    zs(2, 2)
    for half in (1, -1):
        both("x0", -1, half)
        both("x0", 1, half)
    x1(-1)
    x1(1)
    both("y0c", 1)
    y1c()
    both("x0", 2, 1)
    both("x0", 2, -1)
    x1(2)
    both("z3", -1)
    both("z3", 1)
    use(-1, z_rows, True)
    use(1, z_rows, True)
    both("z2", 2)
    z3(2)
    both("y0c", -1)
    use(-1, c_rows)
    use(1, c_rows)
    some_scales = scale_in.at[pl.ds(0, WALK - 1)]
    pltpu.make_async_copy(some_scales, some_scales, small_recv.at[2]).wait()
    scales[y] = jnp.sum(scale_in[...], axis=0)
    to_up = [
        pltpu.make_async_remote_copy(
            src_ref=scales.at[y], dst_ref=scales.at[y],
            send_sem=small_send.at[3], recv_sem=small_recv.at[3],
            device_id=on_y(step), device_id_type=MESH,
        )
        for step in range(1, NY)
    ]
    for copy in to_up:
        copy.start()

    both("x1", -1)
    both("x1", 1)
    use(-1, x_rows)
    use(1, x_rows)
    both("y1c")
    use(2, c_rows, True)
    both("x1", 2)
    use(2, x_rows)
    both("z3", 2)
    use(2, z_rows)
    some_blocks = scales.at[pl.ds(0, NY - 1)]
    pltpu.make_async_copy(some_blocks, some_blocks, small_recv.at[3]).wait()

    def exchange(slot, tile):
        return pltpu.make_async_remote_copy(
            src_ref=own_part.at[slot, tile], dst_ref=other_part.at[slot, tile],
            send_sem=part_send.at[slot, tile], recv_sem=part_recv.at[slot, tile],
            device_id=partner, device_id_type=MESH,
        )

    def mix(slot):
        for block in range(NY):
            mixed[:, block * PTS : (block + 1) * PTS] = (
                current[block] * (scales[block] / (slot + 1).astype(F32))
            ).astype(BF16)

    def points_to_basis(slot):
        mix(slot)
        for pair_of in range(0, TILES, 2):
            columns = slice(pair_of * TILE, (pair_of + 2) * TILE)
            value = dot(mixed[:, :PTS], turned[:PTS, columns])
            for block in range(1, NY):
                points = slice(block * PTS, (block + 1) * PTS)
                value += dot(mixed[:, points], turned[points, columns])
            for tile in (pair_of, pair_of + 1):
                first = (tile - pair_of) * TILE
                own_part[slot, tile] = value[:, first : first + TILE].astype(BF16)
                exchange(slot, tile).start()

    def summed(slot, tile):
        exchange(slot, tile).wait_recv()
        columns = slice(tile * TILE, (tile + 1) * TILE)
        value = (own_part[slot, tile].astype(F32) + other_part[slot, tile].astype(F32)).astype(BF16)
        total[:, columns] = total[:, columns] + value.astype(F32)
        return value

    def one_term(slot, carry):
        points_to_basis(slot)
        for tile in range(0, TILES, 2):
            value = jnp.concatenate([summed(slot, tile), summed(slot, tile + 1)], axis=1)
            for block in range(NY):
                part = dot(value, ip[block, tile * TILE : (tile + 2) * TILE, :])
                current[block] = current[block] + part if tile else part
        return carry

    lax.fori_loop(0, TERMS - 1, one_term, 0)
    last = TERMS - 1
    mix(jnp.int32(last))
    mine = pl.ds(pl.multiple_of(core * COLS, COLS), COLS)
    others = pl.ds(pl.multiple_of((1 - core) * COLS, COLS), COLS)

    def exchange_half(tile):
        return pltpu.make_async_remote_copy(
            src_ref=own_part.at[last, tile, :, others], dst_ref=other_part.at[last, tile, :, others],
            send_sem=part_send.at[last, tile], recv_sem=part_recv.at[last, tile],
            device_id=partner, device_id_type=MESH,
        )

    def begin(step):
        to = at_y(step)
        columns = pl.ds(pl.multiple_of(to * TILE, TILE), TILE)
        own_part[last, to] = dot(mixed[...], turned[:, columns]).astype(BF16)
        exchange_half(to).start()

    def finish(step):
        to = at_y(step)
        exchange_half(to).wait_recv()
        value = own_part[last, to, :, mine].astype(F32) + other_part[last, to, :, mine].astype(F32)
        columns = pl.ds(pl.multiple_of(to * TILE + core * COLS, COLS), COLS)
        row = (total[:, columns] + value.astype(BF16).astype(F32)).astype(BF16)
        if step:
            send_out[to] = row
            pltpu.make_async_remote_copy(
                src_ref=send_out.at[to], dst_ref=recv_out.at[y],
                send_sem=out_send, recv_sem=out_recv,
                device_id=on_y(step), device_id_type=MESH,
            ).start()
        else:
            recv_out[y] = row

    begin(2)
    begin(1)
    begin(3)
    finish(2)
    finish(1)
    begin(0)
    finish(3)
    finish(0)
    for copy in transfers.values():
        copy.wait_send()
    for copy in (*o_up, *o_down, o_across, o_up2, o_down2, o_across_below, o_across_above, o_across_far):
        copy.wait_send()
    pltpu.make_async_copy(some, some, small_send.at[0]).wait()
    pltpu.make_async_copy(some_bias, some_bias, small_send.at[1]).wait()
    pltpu.make_async_copy(some_scales, some_scales, small_send.at[2]).wait()
    pltpu.make_async_copy(some_blocks, some_blocks, small_send.at[3]).wait()
    across.wait_send()
    for slot in range(TERMS):
        for tile in range(TILES):
            (exchange if slot < last else lambda _, to: exchange_half(to))(slot, tile).wait_send()
    some_out = recv_out.at[pl.ds(0, NY - 1)]
    pltpu.make_async_copy(some_out, some_out, out_recv).wait()
    pltpu.make_async_copy(some_out, some_out, out_send).wait()


def assemble(parts, bias_in, out, bias_out):
    for part in range(NY):
        count = WIN if part == NY - 1 else STEP
        out[0, part * STEP : part * STEP + count] = parts[part, :count]
    bias_out[...] = bias_in[...]


N_GATHER = 16 + 18 + 24


def on_device(orbitals, intersection_inv, interp, occ_interp, chol_factors, fields):
    dma = pltpu.SemaphoreType.DMA
    hbm = pl.BlockSpec(memory_space=pltpu.HBM)
    vmem = pl.BlockSpec(memory_space=pltpu.VMEM)
    pieces = pl.pallas_call(
        kernel,
        out_shape=(
            jax.ShapeDtypeStruct((NY, WIN, COLS), BF16),
            jax.ShapeDtypeStruct((WALK, VEC), F32),
        ),
        in_specs=[hbm] * 6,
        out_specs=(vmem, vmem),
        scratch_shapes=[
            pltpu.VMEM((NY, BASIS, PTS), BF16),
            pltpu.VMEM((NY * PTS, BASIS), BF16),
            pltpu.VMEM((CHOL, ROWS, COLS), BF16),
            pltpu.VMEM((ROWS, ROWS), BF16),
            pltpu.VMEM((ROWS, PTS), BF16),
            pltpu.VMEM((PTS, VEC), BF16),
            pltpu.VMEM((WALK, VEC), F32),
            pltpu.VMEM((ROWS, PTS), F32),
            pltpu.VMEM((ROWS, PTS), F32),
            pltpu.VMEM((WALK, 1, PTS), F32),
            pltpu.VMEM((2, WALK, VEC), F32),
            pltpu.VMEM((NY, WALK, VEC), F32),
            pltpu.VMEM((WALK, 1, PTS), F32),
            pltpu.VMEM((WALK, 1, PTS), F32),
            pltpu.VMEM((NY, 1, PTS), F32),
            pltpu.VMEM((NY, WIN, PTS), F32),
            pltpu.VMEM((WIN, NY * PTS), BF16),
            pltpu.VMEM((TERMS, TILES, WIN, TILE), BF16),
            pltpu.VMEM((TERMS, TILES, WIN, TILE), BF16),
            pltpu.VMEM((WIN, BASIS), BF16),
            pltpu.VMEM((WIN, BASIS), F32),
            pltpu.VMEM((NY, WIN, COLS), BF16),
            dma((6,)),
            dma((N_GATHER,)),
            dma((N_GATHER,)),
            dma((10,)),
            dma((10,)),
            dma((5,)),
            dma((5,)),
            dma((TERMS, TILES)),
            dma((TERMS, TILES)),
            dma,
            dma,
            pltpu.SemaphoreType.REGULAR((NZ // 2 + 1,)),
        ],
        compiler_params=pltpu.CompilerParams(
            collective_id=0, has_side_effects=True, vmem_limit_bytes=44 * 1024 * 1024
        ),
    )(
        *(
            pltpu.with_memory_space_constraint(value, pltpu.HBM)
            for value in (orbitals, intersection_inv, interp, occ_interp, chol_factors, fields)
        )
    )
    return pl.pallas_call(
        assemble,
        out_shape=(
            jax.ShapeDtypeStruct((1, ROWS, COLS), BF16),
            jax.ShapeDtypeStruct((WALK, VEC), F32),
        ),
        in_specs=[vmem] * 2,
        out_specs=(vmem, vmem),
        compiler_params=pltpu.CompilerParams(vmem_limit_bytes=8 * 1024 * 1024),
    )(*pieces)


def solution(mesh):
    placed = (
        P("walk", None, "chol"),
        P("walk", None, None),
        P(None, "chol"),
        P(None, "chol"),
        P("chol", "walk"),
        P(None, "walk"),
    )
    return jax.shard_map(
        on_device,
        mesh=mesh,
        in_specs=placed,
        out_specs=(P("walk", None, "chol"), P(None, "walk")),
        check_vma=False,
    )
```
